32 devices in a mesh: gz: 8 (over z, y), gy: 4 (over x, core).
Axes of the slice: x: 2, y: 2, z: 4, core: 2. Of those that a mesh axis runs over, the one named last changes fastest.
Arguments:
- right_side: float32 [8, 16, 256, 512], P(None, 'gz', 'gy'), may hold values from -8 to 8
- diagonal: float32 [16, 256, 512], P('gz', 'gy'), may hold values from 0.1 to 4
Outputs:
- solution: float32 [8, 16, 256, 512], P(None, 'gz', 'gy')
- hessenberg: float32 [24, 32], replicated
The draws below stay inside these ranges and needn't reach their ends.
All inputs are finite; a program needn't handle non-finite values.
Results may differ from the reference program's by a relative error of at most 0.0003.
Values sent between devices are 32-bit elements; how exact they have to be, the bound alone decides.
No kernel may reach another device: no remote copies, remote signals or barrier semaphores. Data moves between devices by JAX's collectives and lax.ppermute only.
A program may use at most 64 MiB of HBM per device.

```python
import math
import jax
import jax.numpy as jnp
from jax import lax

BLK = 8
ITERS = 3
NX = 512
NZ = 16
NY = 256


def level_of(rng, dims, shards, smallest, top_value):
    gain = 1.0
    for axis_at, shards_of in shards:
        draws = jax.random.uniform(jax.random.fold_in(jax.random.fold_in(rng, 6), axis_at), (shards_of,), jnp.float32, smallest / len(shards), top_value / len(shards))
        gain = gain * jnp.repeat(jnp.exp(draws), dims[axis_at] // shards_of).reshape((-1,) + (1,) * (len(dims) - 1 - axis_at))
    return gain


def gaussian(key, shape, deviation, most, split=(), dtype=jnp.bfloat16):
    level = level_of(key, shape, split, -0.22, 0.18) if split else 1.0
    drawn = jax.random.normal(key, shape, jnp.float32) * deviation * level
    return jnp.minimum(jnp.maximum(drawn, -most), most).astype(dtype)


def setup_inputs(seed: int = 0) -> dict:
    streams_of = jax.random.split(jax.random.key(seed), 3)
    return {
        "right_side": gaussian(streams_of[0], (BLK, NZ, NY, NX), 1.0, 8.0, ((1, 8), (2, 4)), jnp.float32),
        "diagonal": jnp.clip(jnp.exp(math.log(4.0) - 3.6888794 * jax.random.uniform(streams_of[1], (NZ, NY, NX), jnp.float32) ** level_of(streams_of[1], (NZ, NY, NX), ((0, 8), (1, 4)), -0.2, 0.2)), 0.1, 4.0),
    }


def apply_op(field, diagonal):
    padded = jnp.pad(field, ((0, 0), (1, 1), (1, 1), (1, 1)))
    beside = padded[:, 2:, 1:-1, 1:-1] + padded[:, :-2, 1:-1, 1:-1]
    beside = beside + padded[:, 1:-1, 2:, 1:-1] + padded[:, 1:-1, :-2, 1:-1]
    beside = beside + padded[:, 1:-1, 1:-1, 2:] + padded[:, 1:-1, 1:-1, :-2]
    return (6.0 + diagonal)[None] * field - beside

def inner(left, right):
    return jnp.dot(left, right.T, precision=lax.Precision.HIGHEST)

def reference(right_side, diagonal):
    shape = right_side.shape
    flat_rhs = right_side.reshape(BLK, -1)
    lower0 = jnp.linalg.cholesky(inner(flat_rhs, flat_rhs))
    basis = [jax.scipy.linalg.solve_triangular(lower0, flat_rhs, lower=True)]
    blocks = []
    for step in range(ITERS):
        work = apply_op(basis[step].reshape(shape), diagonal).reshape(BLK, -1)
        coeff = [inner(work, vec) for vec in basis]
        reduced = work
        for index in range(step + 1):
            reduced = reduced - jnp.dot(coeff[index], basis[index], precision=lax.Precision.HIGHEST)
        lower = jnp.linalg.cholesky(inner(reduced, reduced))
        basis.append(jax.scipy.linalg.solve_triangular(lower, reduced, lower=True))
        row = coeff + [lower] + [jnp.zeros((BLK, BLK), jnp.float32)] * (ITERS - 1 - step)
        blocks.append(jnp.concatenate(row, axis=1))
    hessenberg = jnp.concatenate(blocks, axis=0)
    normal = jnp.dot(hessenberg, hessenberg.T, precision=lax.Precision.HIGHEST)
    factor = jnp.linalg.cholesky(normal)
    target = jnp.dot(hessenberg[:, :BLK], lower0.T, precision=lax.Precision.HIGHEST)
    coeffs = jax.scipy.linalg.cho_solve((factor, True), target)
    stacked = jnp.concatenate(basis[:ITERS], axis=0)
    solution = jnp.dot(coeffs.T, stacked, precision=lax.Precision.HIGHEST)
    return (solution.reshape(shape), hessenberg)
```

```python
import functools
import math

import jax
import jax.numpy as jnp
from jax import lax
from jax.experimental import pallas as pl
from jax.experimental.pallas import tpu as pltpu
from jax.sharding import PartitionSpec as P

ITERS = 3
EDGE = 4
CENTER, SPREAD = 7.6, 2.6
BETA = (0.0, 1.0, 1.5)
HIGHEST = lax.Precision.HIGHEST


def pairs(peers, step):
    return [(i, i + step) for i in range(peers) if 0 <= i + step < peers]


def swap_pairs(peers, bit):
    return [(i, i ^ bit) for i in range(peers)]


def all_sum(array, axes):
    for axis in axes:
        peers = lax.axis_size(axis)
        if peers & (peers - 1):
            array = lax.psum(array, axis)
            continue
        bit = 1
        while bit < peers:
            array = array + lax.ppermute(array, axis, swap_pairs(peers, bit))
            bit *= 2
    return array


def krylov_kernel(keep, got, low_keep, low_got, high_keep, high_got, basis_out, nu_out,
                  x0, x1, x2, x3, acc, sems, out_sems, *, blocks, half, width):
    place = lax.axis_index("gz")
    last = lax.axis_size("gz") - 2
    parity = lax.rem(place, 2)
    rows = half + 2 * EDGE
    mine, other = 2 * parity, 2 - 2 * parity
    copies = []
    for n, (ref, at) in enumerate((
        (keep, 4 + mine), (got, 4 + other), (low_keep, mine), (low_got, other),
        (high_keep, 8 + mine), (high_got, 8 + other),
    )):
        copies.append(pltpu.make_async_copy(ref, x0.at[:, pl.ds(at, 2)], sems.at[n]))
        copies[-1].start()
    for copy in copies:
        copy.wait()

    row = lax.broadcasted_iota(jnp.int32, (rows, width), 0)
    lane = lax.broadcasted_iota(jnp.int32, (rows, width), 1)
    at_y = lax.axis_index("gy")
    no_below = jnp.logical_and(at_y == lax.axis_size("gy") - 1, parity == 1)
    no_above = jnp.logical_and(at_y == 0, parity == 0)
    below = jnp.where(no_below, 0.0, 1.0)
    above = jnp.where(no_above, 0.0, 1.0)
    row_mask = jnp.where(row < half, 1.0, jnp.where(row < half + EDGE, below, above))
    has_low = jnp.where(place >= 2, 1.0, 0.0)
    has_high = jnp.where(place < last, 1.0, 0.0)

    def apply(src, src_at, dst, dst_at, before, before_at, count, first, beta):
        def layer(step, carry):
            index = first + step
            flag = jnp.where(index < 4, has_low, jnp.where(index < 8, 1.0, has_high))
            scale = row_mask * (flag * (1.0 / SPREAD))
            diag = scale * (x0[blocks, index] + (6.0 - CENTER))

            def vector(v, inner):
                mid = src[v, index - src_at]
                beside = src[v, index - src_at - 1] + src[v, index - src_at + 1]
                beside = beside + pltpu.roll(mid, 1, 0) + pltpu.roll(mid, rows - 1, 0)
                beside = beside + jnp.where(lane == 0, 0.0, pltpu.roll(mid, 1, 1))
                beside = beside + jnp.where(lane == width - 1, 0.0, pltpu.roll(mid, width - 1, 1))
                value = diag * mid - scale * beside
                if beta:
                    value = value - beta * before[v, index - before_at]
                dst[v, index - dst_at] = value
                return inner

            return lax.fori_loop(0, blocks, vector, carry)

        lax.fori_loop(0, count, layer, 0)

    apply(x0, 0, x1, 2, None, 0, 8, 2, 0.0)
    apply(x1, 2, x2, 3, x0, 0, 6, 3, BETA[1])
    outs = []
    for n, (ref, at) in enumerate(((x0, 4), (x1, 2), (x2, 1))):
        outs.append(pltpu.make_async_copy(
            ref.at[pl.ds(0, blocks), pl.ds(at, 4), pl.ds(0, half)], basis_out.at[n], out_sems.at[n]))
        outs[-1].start()
    apply(x2, 3, x3, 4, x1, 2, 4, 4, BETA[2])

    held = ((x0, 4), (x1, 2), (x2, 1), (x3, 0))
    tiles = half // 8
    chunks = width // 128
    upper = [(v, w) for v in range(blocks) for w in range(v, blocks)]
    for m in range(2 * ITERS + 1):
        (left, left_at), (right, right_at) = held[m // 2], held[(m + 1) // 2]

        def spot(step, sums, left=left, left_at=left_at, right=right, right_at=right_at):
            layer = step // tiles
            at = pl.multiple_of((step % tiles) * 8, 8)
            sums = list(sums)
            for c in range(chunks):
                lanes = pl.ds(128 * c, 128)
                rights = [right[w, layer + right_at, pl.ds(at, 8), lanes] for w in range(blocks)]
                for v in range(blocks):
                    if left is right:
                        one = rights[v]
                    else:
                        one = left[v, layer + left_at, pl.ds(at, 8), lanes]
                    for n, (a, b) in enumerate(upper):
                        if a == v:
                            sums[n] = sums[n] + one * rights[b]
            return tuple(sums)

        zeros = tuple(jnp.zeros((8, 128), jnp.float32) for _ in upper)
        sums = lax.fori_loop(0, 4 * tiles, spot, zeros)
        for n, (v, w) in enumerate(upper):
            total = jnp.sum(sums[n], axis=0, keepdims=True)
            acc[pl.ds(m * blocks * blocks + v * blocks + w, 1), :] = total
            if v != w:
                acc[pl.ds(m * blocks * blocks + w * blocks + v, 1), :] = total
    nu_out[...] = lax.dot_general(
        jnp.ones((8, 128), jnp.float32), acc[...], (((1,), (1,)), ((), ())),
        precision=HIGHEST, preferred_element_type=jnp.float32)
    for copy in outs:
        copy.wait()


def krylov(pieces, blocks, half, width):
    rows = half + 2 * EDGE
    moments = (2 * ITERS + 1) * blocks * blocks
    padded = -(-moments // 128) * 128
    hbm = pl.BlockSpec(memory_space=pl.ANY)
    return pl.pallas_call(
        functools.partial(krylov_kernel, blocks=blocks, half=half, width=width),
        out_shape=(
            jax.ShapeDtypeStruct((ITERS, blocks, 4, half, width), jnp.float32),
            jax.ShapeDtypeStruct((8, moments), jnp.float32),
        ),
        in_specs=[hbm] * 6,
        out_specs=(hbm, pl.BlockSpec(memory_space=pltpu.VMEM)),
        scratch_shapes=[
            pltpu.VMEM((blocks + 1, 12, rows, width), jnp.float32),
            pltpu.VMEM((blocks, 8, rows, width), jnp.float32),
            pltpu.VMEM((blocks, 6, rows, width), jnp.float32),
            pltpu.VMEM((blocks, 4, rows, width), jnp.float32),
            pltpu.VMEM((moments, 128), jnp.float32),
            pltpu.SemaphoreType.DMA((6,)),
            pltpu.SemaphoreType.DMA((ITERS,)),
        ],
        compiler_params=pltpu.CompilerParams(vmem_limit_bytes=60 << 20),
        name="krylov",
    )(*pieces)


def combine_kernel(at, weights, basis, out, *, blocks, width):
    chunks = width // 128
    sums = [[None] * chunks for _ in range(blocks)]
    for k in range(ITERS):
        for v in range(blocks):
            parts = [basis[k, v, 0, :, 128 * c:128 * c + 128] for c in range(chunks)]
            for w in range(blocks):
                scale = weights[k * blocks + v, w]
                for c in range(chunks):
                    term = scale * parts[c]
                    sums[w][c] = term if sums[w][c] is None else sums[w][c] + term
    for w in range(blocks):
        for c in range(chunks):
            out[w, 0, :, 128 * c:128 * c + 128] = sums[w][c]


def combine(at, weights, basis, half, width):
    blocks = basis.shape[1]
    return pl.pallas_call(
        functools.partial(combine_kernel, blocks=blocks, width=width),
        out_shape=jax.ShapeDtypeStruct((blocks, 2, half, width), jnp.float32),
        grid_spec=pltpu.PrefetchScalarGridSpec(
            num_scalar_prefetch=2,
            grid=(2, half // 8),
            in_specs=[pl.BlockSpec((ITERS, blocks, 1, 8, width), lambda l, t, at, e: (0, 0, at[0] + l, t, 0))],
            out_specs=pl.BlockSpec((blocks, 1, 8, width), lambda l, t, at, e: (0, l, t, 0)),
        ),
        name="combine",
    )(at, weights, basis)


def dense(nu, blocks):
    b1, b2 = BETA[1], BETA[2]
    g02 = nu[2] - b1 * nu[0]
    g03 = nu[3] - b2 * nu[1]
    g13 = nu[4] + b1 * g02 - b2 * nu[2]
    gram = jnp.concatenate([
        jnp.concatenate([nu[0], nu[1], g02, g03], axis=1),
        jnp.concatenate([nu[1], nu[2], nu[3], g13], axis=1),
        jnp.concatenate([g02, nu[3], nu[4], nu[5]], axis=1),
        jnp.concatenate([g03, g13, nu[5], nu[6]], axis=1),
    ], axis=0)
    size = ITERS * blocks
    factor = jnp.linalg.cholesky(gram)
    inverse = jax.scipy.linalg.solve_triangular(
        factor[:size, :size], jnp.eye(size, dtype=jnp.float32), lower=True)
    flat = factor.reshape(ITERS + 1, blocks, size + blocks)
    shifted = [SPREAD * flat[k + 1] + CENTER * flat[k]
               + (SPREAD * BETA[k] * flat[k - 1] if BETA[k] else 0.0) for k in range(ITERS)]
    hessenberg = jnp.dot(inverse, jnp.concatenate(shifted, axis=0), precision=HIGHEST)
    row = lax.broadcasted_iota(jnp.int32, hessenberg.shape, 0) // blocks
    col = lax.broadcasted_iota(jnp.int32, hessenberg.shape, 1) // blocks
    hessenberg = jnp.where(col <= row + 1, hessenberg, 0.0)
    normal = jnp.dot(hessenberg, hessenberg.T, precision=HIGHEST)
    target = jnp.dot(hessenberg[:, :blocks], factor[:blocks, :blocks].T, precision=HIGHEST)
    coeffs = jax.scipy.linalg.cho_solve((jnp.linalg.cholesky(normal), True), target)
    weights = jnp.dot(inverse.T, coeffs, precision=HIGHEST)
    return hessenberg, weights


def body(right_side, diagonal):
    blocks, layers, ny, width = right_side.shape
    half = ny // 2
    peers_z, peers_y = lax.axis_size("gz"), lax.axis_size("gy")
    parity = lax.axis_index("gz") % 2
    field = jnp.concatenate([right_side, diagonal[None]], axis=0)
    above = lax.ppermute(field[:, :, ny - EDGE:], "gy", pairs(peers_y, 1))
    under = lax.ppermute(field[:, :, :EDGE], "gy", pairs(peers_y, -1))
    first = jnp.concatenate([field[:, :, :half + EDGE], above], axis=2)
    second = jnp.concatenate([field[:, :, half:], under, field[:, :, half - EDGE:half]], axis=2)
    keep = jnp.where(parity == 0, first, second)
    send = jnp.where(parity == 0, second, first)
    got = lax.ppermute(send, "gz", swap_pairs(peers_z, 1))
    low_keep = lax.ppermute(keep, "gz", pairs(peers_z, 2))
    high_keep = lax.ppermute(keep, "gz", pairs(peers_z, -2))
    low_got = lax.ppermute(got, "gz", pairs(peers_z, 2))
    high_got = lax.ppermute(got, "gz", pairs(peers_z, -2))
    basis, nu = krylov((keep, got, low_keep, low_got, high_keep, high_got), blocks, half, width)
    nu = all_sum(nu[:1], ("gy", "gz")).reshape(2 * ITERS + 1, blocks, blocks)
    hessenberg, weights = dense(nu, blocks)
    mine = (2 * parity).astype(jnp.int32)
    theirs = combine((2 - mine)[None], weights, basis, half, width)
    back = lax.ppermute(theirs, "gz", swap_pairs(peers_z, 1))
    own = combine(mine[None], weights, basis, half, width)
    upper = jnp.where(parity == 0, own, back)
    lower = jnp.where(parity == 0, back, own)
    return jnp.concatenate([upper, lower], axis=2), hessenberg


def solution(mesh):
    in_specs = (P(None, "gz", "gy", None), P("gz", "gy", None))
    out_specs = (P(None, "gz", "gy", None), P())
    return jax.shard_map(body, mesh=mesh, in_specs=in_specs, out_specs=out_specs, check_vma=False)
```

```python
import functools
import math

import jax
import jax.numpy as jnp
from jax import lax
from jax.experimental import pallas as pl
from jax.experimental.pallas import tpu as pltpu
from jax.sharding import PartitionSpec as P

ITERS = 3
EDGE = 4
CENTER, SPREAD = 7.6, 2.6
BETA = (0.0, 1.0, 1.5)
HIGHEST = lax.Precision.HIGHEST


def pairs(peers, step):
    return [(i, i + step) for i in range(peers) if 0 <= i + step < peers]


def swap_pairs(peers, bit):
    return [(i, i ^ bit) for i in range(peers)]


def all_sum(array, axes):
    for axis in axes:
        peers = lax.axis_size(axis)
        if peers & (peers - 1):
            array = lax.psum(array, axis)
            continue
        bit = 1
        while bit < peers:
            array = array + lax.ppermute(array, axis, swap_pairs(peers, bit))
            bit *= 2
    return array


def krylov_kernel(*refs, blocks, half, width):
    (layers, (basis_out, nu_out, x0, x1, x2, x3, acc, sems, out_sems)) = (refs[:10], refs[10:])
    place = lax.axis_index("gz")
    last = lax.axis_size("gz") - 2
    parity = lax.rem(place, 2)
    rows = half + 2 * EDGE
    copies = []
    for n, ref in enumerate(layers):
        copies.append(pltpu.make_async_copy(ref, x0.at[:, n], sems.at[n]))
        copies[-1].start()
    for copy in copies:
        copy.wait()

    row = lax.broadcasted_iota(jnp.int32, (rows, width), 0)
    lane = lax.broadcasted_iota(jnp.int32, (rows, width), 1)
    at_y = lax.axis_index("gy")
    no_below = jnp.logical_and(at_y == lax.axis_size("gy") - 1, parity == 1)
    no_above = jnp.logical_and(at_y == 0, parity == 0)
    below = jnp.where(no_below, 0.0, 1.0)
    above = jnp.where(no_above, 0.0, 1.0)
    row_mask = jnp.where(row < half, 1.0, jnp.where(row < half + EDGE, below, above))
    downward = jnp.where(place >= 2, 1.0, 0.0)
    upward = jnp.where(place < last, 1.0, 0.0)
    has_low = jnp.where(parity == 0, downward, upward)
    has_high = jnp.where(parity == 0, upward, downward)

    def apply(src, src_at, dst, dst_at, before, before_at, count, first, beta):
        def layer(step, carry):
            index = first + step
            flag = jnp.where(index < 3, has_low, jnp.where(index < 7, 1.0, has_high))
            scale = row_mask * (flag * (1.0 / SPREAD))
            diag = scale * (x0[blocks, index] + (6.0 - CENTER))

            def vector(v, inner):
                mid = src[v, index - src_at]
                beside = src[v, index - src_at - 1] + src[v, index - src_at + 1]
                beside = beside + pltpu.roll(mid, 1, 0) + pltpu.roll(mid, rows - 1, 0)
                beside = beside + jnp.where(lane == 0, 0.0, pltpu.roll(mid, 1, 1))
                beside = beside + jnp.where(lane == width - 1, 0.0, pltpu.roll(mid, width - 1, 1))
                value = diag * mid - scale * beside
                if beta:
                    value = value - beta * before[v, index - before_at]
                dst[v, index - dst_at] = value
                return inner

            return lax.fori_loop(0, blocks, vector, carry)

        lax.fori_loop(0, count, layer, 0)

    apply(x0, 0, x1, 1, None, 0, 8, 1, 0.0)
    apply(x1, 1, x2, 2, x0, 0, 6, 2, BETA[1])
    outs = []
    for n, (ref, at) in enumerate(((x0, 3), (x1, 2), (x2, 1))):
        outs.append(pltpu.make_async_copy(
            ref.at[pl.ds(0, blocks), pl.ds(at, 4), pl.ds(0, half)], basis_out.at[n], out_sems.at[n]))
        outs[-1].start()
    apply(x2, 2, x3, 3, x1, 1, 4, 3, BETA[2])

    held = ((x0, 3), (x1, 2), (x2, 1), (x3, 0))
    tiles = half // 8
    chunks = width // 128
    upper = [(v, w) for v in range(blocks) for w in range(v, blocks)]
    for m in range(2 * ITERS + 1):
        (left, left_at), (right, right_at) = held[m // 2], held[(m + 1) // 2]

        def spot(step, sums, left=left, left_at=left_at, right=right, right_at=right_at):
            layer = step // tiles
            at = pl.multiple_of((step % tiles) * 8, 8)
            sums = list(sums)
            for c in range(chunks):
                lanes = pl.ds(128 * c, 128)
                rights = [right[w, layer + right_at, pl.ds(at, 8), lanes] for w in range(blocks)]
                for v in range(blocks):
                    if left is right:
                        one = rights[v]
                    else:
                        one = left[v, layer + left_at, pl.ds(at, 8), lanes]
                    for n, (a, b) in enumerate(upper):
                        if a == v:
                            sums[n] = sums[n] + one * rights[b]
            return tuple(sums)

        zeros = tuple(jnp.zeros((8, 128), jnp.float32) for _ in upper)
        sums = lax.fori_loop(0, 4 * tiles, spot, zeros)
        for n, (v, w) in enumerate(upper):
            total = jnp.sum(sums[n], axis=0, keepdims=True)
            acc[pl.ds(m * blocks * blocks + v * blocks + w, 1), :] = total
            if v != w:
                acc[pl.ds(m * blocks * blocks + w * blocks + v, 1), :] = total
    nu_out[...] = lax.dot_general(
        jnp.ones((8, 128), jnp.float32), acc[...], (((1,), (1,)), ((), ())),
        precision=HIGHEST, preferred_element_type=jnp.float32)
    for copy in outs:
        copy.wait()


def krylov(pieces, blocks, half, width):
    rows = half + 2 * EDGE
    moments = (2 * ITERS + 1) * blocks * blocks
    padded = -(-moments // 128) * 128
    hbm = pl.BlockSpec(memory_space=pl.ANY)
    return pl.pallas_call(
        functools.partial(krylov_kernel, blocks=blocks, half=half, width=width),
        out_shape=(
            jax.ShapeDtypeStruct((ITERS, blocks, 4, half, width), jnp.float32),
            jax.ShapeDtypeStruct((8, moments), jnp.float32),
        ),
        in_specs=[hbm] * 10,
        out_specs=(hbm, pl.BlockSpec(memory_space=pltpu.VMEM)),
        scratch_shapes=[
            pltpu.VMEM((blocks + 1, 10, rows, width), jnp.float32),
            pltpu.VMEM((blocks, 8, rows, width), jnp.float32),
            pltpu.VMEM((blocks, 6, rows, width), jnp.float32),
            pltpu.VMEM((blocks, 4, rows, width), jnp.float32),
            pltpu.VMEM((moments, 128), jnp.float32),
            pltpu.SemaphoreType.DMA((10,)),
            pltpu.SemaphoreType.DMA((ITERS,)),
        ],
        compiler_params=pltpu.CompilerParams(vmem_limit_bytes=60 << 20),
        name="krylov",
    )(*pieces)


def combine_kernel(weights, basis, out, *, blocks, width):
    chunks = width // 128
    sums = [[None] * chunks for _ in range(blocks)]
    for k in range(ITERS):
        for v in range(blocks):
            parts = [basis[k, v, 0, :, 128 * c:128 * c + 128] for c in range(chunks)]
            for w in range(blocks):
                scale = weights[k * blocks + v, w]
                for c in range(chunks):
                    term = scale * parts[c]
                    sums[w][c] = term if sums[w][c] is None else sums[w][c] + term
    for w in range(blocks):
        for c in range(chunks):
            out[w, 0, :, 128 * c:128 * c + 128] = sums[w][c]


def combine(first, weights, basis, half, width):
    blocks = basis.shape[1]
    return pl.pallas_call(
        functools.partial(combine_kernel, blocks=blocks, width=width),
        out_shape=jax.ShapeDtypeStruct((blocks, 2, half, width), jnp.float32),
        grid=(2, half // 8),
        in_specs=[
            pl.BlockSpec(memory_space=pltpu.SMEM),
            pl.BlockSpec((ITERS, blocks, 1, 8, width), lambda l, t: (0, 0, first + l, t, 0)),
        ],
        out_specs=pl.BlockSpec((blocks, 1, 8, width), lambda l, t: (0, l, t, 0)),
        name="combine",
    )(weights, basis)


def dense(nu, blocks):
    b1, b2 = BETA[1], BETA[2]
    g02 = nu[2] - b1 * nu[0]
    g03 = nu[3] - b2 * nu[1]
    g13 = nu[4] + b1 * g02 - b2 * nu[2]
    gram = jnp.concatenate([
        jnp.concatenate([nu[0], nu[1], g02, g03], axis=1),
        jnp.concatenate([nu[1], nu[2], nu[3], g13], axis=1),
        jnp.concatenate([g02, nu[3], nu[4], nu[5]], axis=1),
        jnp.concatenate([g03, g13, nu[5], nu[6]], axis=1),
    ], axis=0)
    size = ITERS * blocks
    factor = jnp.linalg.cholesky(gram)
    inverse = jax.scipy.linalg.solve_triangular(
        factor[:size, :size], jnp.eye(size, dtype=jnp.float32), lower=True)
    flat = factor.reshape(ITERS + 1, blocks, size + blocks)
    shifted = [SPREAD * flat[k + 1] + CENTER * flat[k]
               + (SPREAD * BETA[k] * flat[k - 1] if BETA[k] else 0.0) for k in range(ITERS)]
    hessenberg = jnp.dot(inverse, jnp.concatenate(shifted, axis=0), precision=HIGHEST)
    row = lax.broadcasted_iota(jnp.int32, hessenberg.shape, 0) // blocks
    col = lax.broadcasted_iota(jnp.int32, hessenberg.shape, 1) // blocks
    hessenberg = jnp.where(col <= row + 1, hessenberg, 0.0)
    normal = jnp.dot(hessenberg, hessenberg.T, precision=HIGHEST)
    target = jnp.dot(hessenberg[:, :blocks], factor[:blocks, :blocks].T, precision=HIGHEST)
    coeffs = jax.scipy.linalg.cho_solve((jnp.linalg.cholesky(normal), True), target)
    weights = jnp.dot(inverse.T, coeffs, precision=HIGHEST)
    return hessenberg, weights


def body(right_side, diagonal):
    blocks, layers, ny, width = right_side.shape
    half = ny // 2
    peers_z, peers_y = lax.axis_size("gz"), lax.axis_size("gy")
    even = lax.axis_index("gz") % 2 == 0
    field = jnp.concatenate([right_side, diagonal[None]], axis=0)
    above = lax.ppermute(field[:, :, ny - EDGE:], "gy", pairs(peers_y, 1))
    under = lax.ppermute(field[:, :, :EDGE], "gy", pairs(peers_y, -1))
    first = jnp.concatenate([field[:, :, :half + EDGE], above], axis=2)
    second = jnp.concatenate([field[:, :, half:], under, field[:, :, half - EDGE:half]], axis=2)

    swap = swap_pairs(peers_z, 1)
    inward = [(i, j) for i, j in pairs(peers_z, 2) if i % 2 == 0] + [(i, j) for i, j in pairs(peers_z, -2) if i % 2]
    outward = [(j, i) for i, j in inward]
    send_near = jnp.where(even, second[:, 1], first[:, 0])
    send_far = jnp.where(even, second[:, 0], first[:, 1])
    keep_near = jnp.where(even, first[:, 1], second[:, 0])
    keep_far = jnp.where(even, first[:, 0], second[:, 1])
    got_near = lax.ppermute(send_near, "gz", swap)
    in_one = lax.ppermute(keep_near, "gz", inward)
    out_one = lax.ppermute(keep_far, "gz", outward)
    got_far = lax.ppermute(send_far, "gz", swap)
    out_two = lax.ppermute(keep_near, "gz", outward)
    in_two = lax.ppermute(got_near, "gz", inward)
    out_three = lax.ppermute(got_near, "gz", outward)
    in_three = lax.ppermute(got_far, "gz", inward)
    pieces = (in_one, in_two, in_three, keep_far, keep_near, got_near, got_far, out_one, out_two, out_three)
    basis, nu = krylov(pieces, blocks, half, width)
    nu = all_sum(nu[:1], ("gy", "gz")).reshape(2 * ITERS + 1, blocks, blocks)
    hessenberg, weights = dense(nu, blocks)
    theirs = combine(2, weights, basis, half, width)
    back = lax.ppermute(theirs, "gz", swap)
    own = combine(0, weights, basis, half, width)
    parts = [[jnp.where(even, own[:, 0], back[:, 0]), jnp.where(even, back[:, 1], own[:, 1])],
             [jnp.where(even, own[:, 1], back[:, 1]), jnp.where(even, back[:, 0], own[:, 0])]]
    whole = jnp.stack([jnp.concatenate(part, axis=1) for part in parts], axis=1)
    return whole, hessenberg


def solution(mesh):
    in_specs = (P(None, "gz", "gy", None), P("gz", "gy", None))
    out_specs = (P(None, "gz", "gy", None), P())
    return jax.shard_map(body, mesh=mesh, in_specs=in_specs, out_specs=out_specs, check_vma=False)
```

```python
import functools

import jax
import jax.numpy as jnp
import numpy as np
from jax import lax
from jax.experimental import pallas as pl
from jax.experimental.pallas import tpu as pltpu
from jax.sharding import PartitionSpec as P

ITERS = 3
EDGE = 4
CENTER, SPREAD = 7.6, 2.6
BETA = (0.0, 1.0, 1.5)
HIGHEST = lax.Precision.HIGHEST


def pairs(peers, step):
    return [(i, i + step) for i in range(peers) if 0 <= i + step < peers]


def swap_pairs(peers, bit):
    return [(i, i ^ bit) for i in range(peers)]


def all_sum(array, axes):
    for axis in axes:
        peers = lax.axis_size(axis)
        if peers & (peers - 1):
            array = lax.psum(array, axis)
            continue
        bit = 1
        while bit < peers:
            array = array + lax.ppermute(array, axis, swap_pairs(peers, bit))
            bit *= 2
    return array


def row_masks(half, width):
    rows = half + 2 * EDGE
    parity = lax.rem(lax.axis_index("gz"), 2)
    at_y = lax.axis_index("gy")
    no_below = jnp.logical_and(at_y == lax.axis_size("gy") - 1, parity == 1)
    no_above = jnp.logical_and(at_y == 0, parity == 0)
    row = lax.broadcasted_iota(jnp.int32, (rows, width), 0)
    below = jnp.where(no_below, 0.0, 1.0)
    above = jnp.where(no_above, 0.0, 1.0)
    return jnp.where(row < half, 1.0, jnp.where(row < half + EDGE, below, above))


def side_flags():
    place = lax.axis_index("gz")
    parity = lax.rem(place, 2)
    downward = jnp.where(place >= 2, 1.0, 0.0)
    upward = jnp.where(place < lax.axis_size("gz") - 2, 1.0, 0.0)
    return (jnp.where(parity == 0, downward, upward), jnp.where(parity == 0, upward, downward))


def set_scales(scale_ref, diag_ref, fields, blocks, slots, half, width):
    scale_ref[...] = row_masks(half, width) * (1.0 / SPREAD)
    low, high = side_flags()
    for slot, (layer, ref) in enumerate(zip(slots, fields)):
        value = scale_ref[...] * (ref[blocks] + (6.0 - CENTER))
        if layer < 4:
            value = value * low
        if layer > 7:
            value = value * high
        diag_ref[slot] = value


def step_of(scale, diag, low, mid, high, before, beta, flag=None):
    rows, width = mid.shape
    lane = lax.broadcasted_iota(jnp.int32, (rows, width), 1)
    beside = low + high
    beside = beside + pltpu.roll(mid, 1, 0) + pltpu.roll(mid, rows - 1, 0)
    beside = beside + jnp.where(lane == 0, 0.0, pltpu.roll(mid, 1, 1))
    beside = beside + jnp.where(lane == width - 1, 0.0, pltpu.roll(mid, width - 1, 1))
    if flag is not None:
        scale = scale * flag
    value = diag * mid - scale * beside
    if beta:
        value = value - beta * before
    return value


def gram_part(acc, views, moment, layers, blocks, half, width, start):
    left, right = views[moment // 2], views[(moment + 1) // 2]
    upper = [(v, w) for v in range(blocks) for w in range(v, blocks)]

    def spot(step, sums):
        at = pl.multiple_of(step * 8, 8)
        sums = list(sums)
        for layer in layers:
            for c in range(width // 128):
                lanes = pl.ds(128 * c, 128)
                rights = [right[layer][w, pl.ds(at, 8), lanes] for w in range(blocks)]
                for v in range(blocks):
                    one = rights[v] if left is right else left[layer][v, pl.ds(at, 8), lanes]
                    for n, (a, b) in enumerate(upper):
                        if a == v:
                            sums[n] = sums[n] + one * rights[b]
        return tuple(sums)

    zeros = tuple(jnp.zeros((8, 128), jnp.float32) for _ in upper)
    sums = lax.fori_loop(0, half // 8, spot, zeros)
    base = moment * len(upper)
    for n in range(len(upper)):
        acc[base + n] = sums[n] if start is None else sums[n] + start[base + n]


EARLY = {0: (4, 5, 6, 7), 1: (5, 6, 7), 2: (5, 6, 7), 3: (6, 7), 4: (6, 7)}
LATE = {1: (4,), 2: (4,), 3: (4, 5), 4: (4, 5), 5: (4, 5, 6, 7), 6: (4, 5, 6, 7)}


def early_kernel(*refs, blocks, half, width):
    fields = dict(zip((4, 5, 6, 7, 8, 9), refs[:6]))
    x1, x2, acc, scale_ref, diag_ref = refs[6:]
    slots = (5, 6, 7, 8)
    set_scales(scale_ref, diag_ref, [fields[n] for n in slots], blocks, slots, half, width)
    flag = side_flags()[1]

    def vector(v, carry):
        for slot, n in enumerate(slots):
            x1[slot, v] = step_of(
                scale_ref[...], diag_ref[slot], fields[n - 1][v], fields[n][v], fields[n + 1][v],
                None, 0.0, flag if n == 8 else None)
        for slot, n in enumerate((6, 7)):
            x2[slot, v] = step_of(
                scale_ref[...], diag_ref[n - 5], x1[n - 6, v], x1[n - 5, v], x1[n - 4, v],
                fields[n][v], BETA[1])
        return carry

    lax.fori_loop(0, blocks, vector, 0)
    views = (fields, {n: x1.at[n - 5] for n in slots}, {n: x2.at[n - 6] for n in (6, 7)})
    for moment, layers in EARLY.items():
        gram_part(acc, views, moment, layers, blocks, half, width, None)


def late_kernel(*refs, blocks, half, width):
    fields = dict(zip(range(1, 11), refs[:10]))
    near1, near2, start, x1, x2, nu_out, far1, far2, x3, acc, scale_ref, diag_ref = refs[10:]
    slots = tuple(range(2, 10))
    set_scales(scale_ref, diag_ref, [fields[n] for n in slots], blocks, slots, half, width)
    low, high = side_flags()
    one = {2: far1.at[0], 3: far1.at[1], 4: x1, 9: far1.at[2], **{n: near1.at[n - 5] for n in (5, 6, 7, 8)}}
    two = {3: far2.at[0], 4: x2.at[0], 5: x2.at[1], 6: near2.at[0], 7: near2.at[1], 8: far2.at[1]}
    three = {n: x3.at[n - 4] for n in (4, 5, 6, 7)}

    def flag_of(n):
        return low if n < 4 else high if n > 7 else None

    def vector(v, carry):
        for n in (2, 3, 4, 9):
            one[n][v] = step_of(
                scale_ref[...], diag_ref[n - 2], fields[n - 1][v], fields[n][v], fields[n + 1][v],
                None, 0.0, flag_of(n))
        for n in (3, 4, 5, 8):
            two[n][v] = step_of(
                scale_ref[...], diag_ref[n - 2], one[n - 1][v], one[n][v], one[n + 1][v],
                fields[n][v], BETA[1], flag_of(n))
        for n in (4, 5, 6, 7):
            three[n][v] = step_of(
                scale_ref[...], diag_ref[n - 2], two[n - 1][v], two[n][v], two[n + 1][v],
                one[n][v], BETA[2])
        return carry

    lax.fori_loop(0, blocks, vector, 0)
    views = (fields, one, two, three)
    upper = [(v, w) for v in range(blocks) for w in range(v, blocks)]
    acc[pl.ds(0, len(upper))] = start[pl.ds(0, len(upper))]
    for moment, layers in LATE.items():
        gram_part(acc, views, moment, layers, blocks, half, width, start if moment in EARLY else None)
    total = jnp.sum(acc[...], axis=1)
    nu_out[...] = lax.dot_general(
        jnp.ones((8, 128), jnp.float32), total, (((1,), (1,)), ((), ())),
        precision=HIGHEST, preferred_element_type=jnp.float32)


def krylov(pieces, blocks, half, width):
    rows = half + 2 * EDGE
    moments = 2 * ITERS + 1
    count = blocks * (blocks + 1) // 2
    vmem = pl.BlockSpec(memory_space=pltpu.VMEM)
    sizes = dict(blocks=blocks, half=half, width=width)
    layer = (blocks, rows, width)
    cells = blocks * rows * width

    def out(*shape):
        return jax.ShapeDtypeStruct(shape, jnp.float32)

    near1, near2, start = pl.pallas_call(
        functools.partial(early_kernel, **sizes),
        out_shape=(out(4, *layer), out(2, *layer), out(len(EARLY) * count, 8, 128)),
        in_specs=[vmem] * 6,
        out_specs=(vmem,) * 3,
        scratch_shapes=[pltpu.VMEM((rows, width), jnp.float32), pltpu.VMEM((4, rows, width), jnp.float32)],
        compiler_params=pltpu.CompilerParams(vmem_limit_bytes=20 << 20),
        cost_estimate=pl.CostEstimate(flops=400 * cells, bytes_accessed=16 * cells, transcendentals=0),
        name="early",
    )(*pieces[3:9])
    x1, x2, nu = pl.pallas_call(
        functools.partial(late_kernel, **sizes),
        out_shape=(out(*layer), out(2, *layer), out(8, moments * count)),
        in_specs=[vmem] * 13,
        out_specs=(vmem,) * 3,
        scratch_shapes=[
            pltpu.VMEM((3, *layer), jnp.float32),
            pltpu.VMEM((2, *layer), jnp.float32),
            pltpu.VMEM((4, *layer), jnp.float32),
            pltpu.VMEM((moments * count, 8, 128), jnp.float32),
            pltpu.VMEM((rows, width), jnp.float32),
            pltpu.VMEM((8, rows, width), jnp.float32),
        ],
        compiler_params=pltpu.CompilerParams(vmem_limit_bytes=34 << 20),
        cost_estimate=pl.CostEstimate(flops=400 * cells, bytes_accessed=16 * cells, transcendentals=0),
        name="late",
    )(*pieces, near1, near2, start)
    return near1, near2, x1, x2, nu


def combine_kernel(weights, *refs, blocks, half, width, places):
    out = refs[-1]
    for layer in range(2):
        terms = [(refs[ref].at[at] if at is not None else refs[ref]) for ref, at in places[layer]]

        def tile(step, carry, terms=terms, layer=layer):
            at = pl.multiple_of(step * 8, 8)
            for c in range(width // 128):
                lanes = pl.ds(128 * c, 128)
                sums = [None] * blocks
                for k, term in enumerate(terms):
                    for v in range(blocks):
                        part = term[v, pl.ds(at, 8), lanes]
                        for w in range(blocks):
                            value = weights[k * blocks + v, w] * part
                            sums[w] = value if sums[w] is None else sums[w] + value
                for w in range(blocks):
                    out[w, layer, pl.ds(at, 8), lanes] = sums[w]
            return carry

        lax.fori_loop(0, half // 8, tile, 0)


def combine(weights, arrays, places, blocks, half, width):
    vmem = pl.BlockSpec(memory_space=pltpu.VMEM)
    return pl.pallas_call(
        functools.partial(combine_kernel, blocks=blocks, half=half, width=width, places=places),
        out_shape=jax.ShapeDtypeStruct((blocks, 2, half, width), jnp.float32),
        in_specs=[pl.BlockSpec(memory_space=pltpu.SMEM)] + [vmem] * len(arrays),
        out_specs=vmem,
        compiler_params=pltpu.CompilerParams(vmem_limit_bytes=16 << 20),
        name="combine",
    )(weights, *arrays)


def full_moments(nu, blocks):
    count = blocks * (blocks + 1) // 2
    pick = np.zeros((count, blocks * blocks), np.float32)
    n = 0
    for v in range(blocks):
        for w in range(v, blocks):
            pick[n, v * blocks + w] = pick[n, w * blocks + v] = 1.0
            n += 1
    full = jnp.dot(nu.reshape(-1, count), pick, precision=HIGHEST)
    return full.reshape(-1, blocks, blocks)


def dense(nu, blocks):
    b1, b2 = BETA[1], BETA[2]
    g02 = nu[2] - b1 * nu[0]
    g03 = nu[3] - b2 * nu[1]
    g13 = nu[4] + b1 * g02 - b2 * nu[2]
    gram = jnp.concatenate([
        jnp.concatenate([nu[0], nu[1], g02, g03], axis=1),
        jnp.concatenate([nu[1], nu[2], nu[3], g13], axis=1),
        jnp.concatenate([g02, nu[3], nu[4], nu[5]], axis=1),
        jnp.concatenate([g03, g13, nu[5], nu[6]], axis=1),
    ], axis=0)
    size = ITERS * blocks
    factor = jnp.linalg.cholesky(gram)
    inverse = jax.scipy.linalg.solve_triangular(
        factor[:size, :size], jnp.eye(size, dtype=jnp.float32), lower=True)
    flat = factor.reshape(ITERS + 1, blocks, size + blocks)
    shifted = [SPREAD * flat[k + 1] + CENTER * flat[k]
               + (SPREAD * BETA[k] * flat[k - 1] if BETA[k] else 0.0) for k in range(ITERS)]
    hessenberg = jnp.dot(inverse, jnp.concatenate(shifted, axis=0), precision=HIGHEST)
    row = lax.broadcasted_iota(jnp.int32, hessenberg.shape, 0) // blocks
    col = lax.broadcasted_iota(jnp.int32, hessenberg.shape, 1) // blocks
    hessenberg = jnp.where(col <= row + 1, hessenberg, 0.0)
    normal = jnp.dot(hessenberg, hessenberg.T, precision=HIGHEST)
    target = jnp.dot(hessenberg[:, :blocks], factor[:blocks, :blocks].T, precision=HIGHEST)
    coeffs = jax.scipy.linalg.cho_solve((jnp.linalg.cholesky(normal), True), target)
    weights = jnp.dot(inverse.T, coeffs, precision=HIGHEST)
    return hessenberg, weights


def body(right_side, diagonal):
    blocks, layers, ny, width = right_side.shape
    half = ny // 2
    peers_z, peers_y = lax.axis_size("gz"), lax.axis_size("gy")
    even = lax.axis_index("gz") % 2 == 0
    field = jnp.concatenate([right_side, diagonal[None]], axis=0)
    above = lax.ppermute(field[:, :, ny - EDGE:], "gy", pairs(peers_y, 1))
    under = lax.ppermute(field[:, :, :EDGE], "gy", pairs(peers_y, -1))
    first = jnp.concatenate([field[:, :, :half + EDGE], above], axis=2)
    second = jnp.concatenate([field[:, :, half:], under, field[:, :, half - EDGE:half]], axis=2)

    swap = swap_pairs(peers_z, 1)
    inward = [(i, j) for i, j in pairs(peers_z, 2) if i % 2 == 0] + [(i, j) for i, j in pairs(peers_z, -2) if i % 2]
    outward = [(j, i) for i, j in inward]
    send_near = jnp.where(even, second[:, 1], first[:, 0])
    send_far = jnp.where(even, second[:, 0], first[:, 1])
    keep_near = jnp.where(even, first[:, 1], second[:, 0])
    keep_far = jnp.where(even, first[:, 0], second[:, 1])
    got_near = lax.ppermute(send_near, "gz", swap)
    in_one = lax.ppermute(keep_near, "gz", inward)
    out_one = lax.ppermute(keep_far, "gz", outward)
    got_far = lax.ppermute(send_far, "gz", swap)
    out_two = lax.ppermute(keep_near, "gz", outward)
    in_two = lax.ppermute(got_near, "gz", inward)
    out_three = lax.ppermute(got_near, "gz", outward)
    in_three = lax.ppermute(got_far, "gz", inward)
    pieces = (in_one, in_two, in_three, keep_far, keep_near, got_near, got_far, out_one, out_two, out_three)
    near1, near2, x1, x2, nu = krylov(pieces, blocks, half, width)
    nu = full_moments(all_sum(nu[:1], ("gy", "gz")), blocks)
    hessenberg, weights = dense(nu, blocks)
    theirs = combine(
        weights, (got_near, got_far, near1, near2),
        (((0, None), (2, 1), (3, 0)), ((1, None), (2, 2), (3, 1))), blocks, half, width)
    back = lax.ppermute(theirs, "gz", swap)
    own = combine(
        weights, (keep_far, keep_near, x1, near1, x2),
        (((0, None), (2, None), (4, 0)), ((1, None), (3, 0), (4, 1))), blocks, half, width)
    parts = [[jnp.where(even, own[:, 0], back[:, 0]), jnp.where(even, back[:, 1], own[:, 1])],
             [jnp.where(even, own[:, 1], back[:, 1]), jnp.where(even, back[:, 0], own[:, 0])]]
    whole = jnp.stack([jnp.concatenate(part, axis=1) for part in parts], axis=1)
    return whole, hessenberg


def solution(mesh):
    in_specs = (P(None, "gz", "gy", None), P("gz", "gy", None))
    out_specs = (P(None, "gz", "gy", None), P())
    return jax.shard_map(body, mesh=mesh, in_specs=in_specs, out_specs=out_specs, check_vma=False)
```

```python
import functools

import jax
import jax.numpy as jnp
import numpy as np
from jax import lax
from jax.experimental import pallas as pl
from jax.experimental.pallas import tpu as pltpu
from jax.sharding import PartitionSpec as P

ITERS = 3
EDGE = 4
CENTER, SPREAD = 7.6, 2.6
BETA = (0.0, 1.0, 1.5)
HIGHEST = lax.Precision.HIGHEST


def pairs(peers, step):
    return [(i, i + step) for i in range(peers) if 0 <= i + step < peers]


def swap_pairs(peers, bit):
    return [(i, i ^ bit) for i in range(peers)]


def all_sum(array, axes):
    peers = 1
    for axis in axes:
        peers *= lax.axis_size(axis)
    spread = jnp.broadcast_to(array[None], (peers, *array.shape))
    return jnp.sum(lax.all_to_all(spread, axes, 0, 0), axis=0)


def row_masks(half, width):
    rows = half + 2 * EDGE
    parity = lax.rem(lax.axis_index("gz"), 2)
    at_y = lax.axis_index("gy")
    no_below = jnp.logical_and(at_y == lax.axis_size("gy") - 1, parity == 1)
    no_above = jnp.logical_and(at_y == 0, parity == 0)
    row = lax.broadcasted_iota(jnp.int32, (rows, width), 0)
    below = jnp.where(no_below, 0.0, 1.0)
    above = jnp.where(no_above, 0.0, 1.0)
    return jnp.where(row < half, 1.0, jnp.where(row < half + EDGE, below, above))


def side_flags():
    place = lax.axis_index("gz")
    parity = lax.rem(place, 2)
    downward = jnp.where(place >= 2, 1.0, 0.0)
    upward = jnp.where(place < lax.axis_size("gz") - 2, 1.0, 0.0)
    return (jnp.where(parity == 0, downward, upward), jnp.where(parity == 0, upward, downward))


def set_scales(scale_ref, diag_ref, fields, blocks, slots, half, width):
    scale_ref[...] = row_masks(half, width) * (1.0 / SPREAD)
    low, high = side_flags()
    for slot, (layer, ref) in enumerate(zip(slots, fields)):
        value = scale_ref[...] * (ref[blocks] + (6.0 - CENTER))
        if layer < 4:
            value = value * low
        if layer > 7:
            value = value * high
        diag_ref[slot] = value


def step_of(scale, diag, low, mid, high, before, beta, flag=None):
    rows, width = mid.shape
    lane = lax.broadcasted_iota(jnp.int32, (rows, width), 1)
    beside = low + high
    beside = beside + pltpu.roll(mid, 1, 0) + pltpu.roll(mid, rows - 1, 0)
    beside = beside + jnp.where(lane == 0, 0.0, pltpu.roll(mid, 1, 1))
    beside = beside + jnp.where(lane == width - 1, 0.0, pltpu.roll(mid, width - 1, 1))
    if flag is not None:
        scale = scale * flag
    value = diag * mid - scale * beside
    if beta:
        value = value - beta * before
    return value


def gram_part(acc, views, moment, layers, blocks, half, width, start):
    left, right = views[moment // 2], views[(moment + 1) // 2]
    upper = [(v, w) for v in range(blocks) for w in range(v, blocks)]

    def spot(step, sums):
        at = pl.multiple_of(step * 8, 8)
        sums = list(sums)
        for layer in layers:
            for c in range(width // 128):
                lanes = pl.ds(128 * c, 128)
                rights = [right[layer][w, pl.ds(at, 8), lanes] for w in range(blocks)]
                for v in range(blocks):
                    one = rights[v] if left is right else left[layer][v, pl.ds(at, 8), lanes]
                    for n, (a, b) in enumerate(upper):
                        if a == v:
                            sums[n] = sums[n] + one * rights[b]
        return tuple(sums)

    zeros = tuple(jnp.zeros((8, 128), jnp.float32) for _ in upper)
    sums = lax.fori_loop(0, half // 8, spot, zeros)
    base = moment * len(upper)
    for n in range(len(upper)):
        acc[base + n] = sums[n] if start is None else sums[n] + start[base + n]


EARLY = {0: (4, 5, 6, 7), 1: (5, 6, 7), 2: (5, 6, 7), 3: (6, 7), 4: (6, 7)}
LATE = {1: (4,), 2: (4,), 3: (4, 5), 4: (4, 5), 5: (4, 5, 6, 7), 6: (4, 5, 6, 7)}


def first_kernel(*refs, blocks, half, width):
    fields = dict(zip((5, 6, 7, 8), refs[:4]))
    x1, sent, scale_ref, diag_ref = refs[4:]
    set_scales(scale_ref, diag_ref, [fields[n] for n in (6, 7)], blocks, (6, 7), half, width)

    def vector(v, carry):
        for slot, n in enumerate((6, 7)):
            value = step_of(
                scale_ref[...], diag_ref[slot], fields[n - 1][v], fields[n][v], fields[n + 1][v], None, 0.0)
            x1[slot, v] = value
            sent[slot, v] = value[:half]
        return carry

    lax.fori_loop(0, blocks, vector, 0)


def early_kernel(*refs, blocks, half, width):
    fields = dict(zip((4, 5, 6, 7, 8, 9), refs[:6]))
    before, x1, x2, near_sent, far_sent, acc, scale_ref, diag_ref = refs[6:]
    slots = (5, 6, 7, 8)
    set_scales(scale_ref, diag_ref, [fields[n] for n in slots], blocks, slots, half, width)
    flag = side_flags()[1]
    one = {5: x1.at[0], 6: before.at[0], 7: before.at[1], 8: x1.at[1]}

    def vector(v, carry):
        for n in (5, 8):
            one[n][v] = step_of(
                scale_ref[...], diag_ref[n - 5], fields[n - 1][v], fields[n][v], fields[n + 1][v],
                None, 0.0, flag if n == 8 else None)
        for slot, (n, sent) in enumerate(((6, near_sent), (7, far_sent))):
            value = step_of(
                scale_ref[...], diag_ref[n - 5], one[n - 1][v], one[n][v], one[n + 1][v],
                fields[n][v], BETA[1])
            x2[slot, v] = value
            sent[v] = value[:half]
        return carry

    lax.fori_loop(0, blocks, vector, 0)
    views = (fields, one, {n: x2.at[n - 6] for n in (6, 7)})
    for moment, layers in EARLY.items():
        gram_part(acc, views, moment, layers, blocks, half, width, None)


def late_kernel(*refs, blocks, half, width):
    fields = dict(zip(range(1, 11), refs[:10]))
    mid1, near1, near2, start, x1, x2, nu_out, far1, far2, x3, acc, scale_ref, diag_ref = refs[10:]
    slots = tuple(range(2, 10))
    set_scales(scale_ref, diag_ref, [fields[n] for n in slots], blocks, slots, half, width)
    low, high = side_flags()
    one = {2: far1.at[0], 3: far1.at[1], 4: x1, 9: far1.at[2],
           5: near1.at[0], 6: mid1.at[0], 7: mid1.at[1], 8: near1.at[1]}
    two = {3: far2.at[0], 4: x2.at[0], 5: x2.at[1], 6: near2.at[0], 7: near2.at[1], 8: far2.at[1]}
    three = {n: x3.at[n - 4] for n in (4, 5, 6, 7)}

    def flag_of(n):
        return low if n < 4 else high if n > 7 else None

    def vector(v, carry):
        for n in (2, 3, 4, 9):
            one[n][v] = step_of(
                scale_ref[...], diag_ref[n - 2], fields[n - 1][v], fields[n][v], fields[n + 1][v],
                None, 0.0, flag_of(n))
        for n in (3, 4, 5, 8):
            two[n][v] = step_of(
                scale_ref[...], diag_ref[n - 2], one[n - 1][v], one[n][v], one[n + 1][v],
                fields[n][v], BETA[1], flag_of(n))
        for n in (4, 5, 6, 7):
            three[n][v] = step_of(
                scale_ref[...], diag_ref[n - 2], two[n - 1][v], two[n][v], two[n + 1][v],
                one[n][v], BETA[2])
        return carry

    lax.fori_loop(0, blocks, vector, 0)
    views = (fields, one, two, three)
    upper = [(v, w) for v in range(blocks) for w in range(v, blocks)]
    acc[pl.ds(0, len(upper))] = start[pl.ds(0, len(upper))]
    for moment, layers in LATE.items():
        gram_part(acc, views, moment, layers, blocks, half, width, start if moment in EARLY else None)
    total = jnp.sum(acc[...], axis=1)
    nu_out[...] = lax.dot_general(
        jnp.ones((8, 128), jnp.float32), total, (((1,), (1,)), ((), ())),
        precision=HIGHEST, preferred_element_type=jnp.float32)


def kernels(blocks, half, width):
    rows = half + 2 * EDGE
    moments = 2 * ITERS + 1
    count = blocks * (blocks + 1) // 2
    vmem = pl.BlockSpec(memory_space=pltpu.VMEM)
    sizes = dict(blocks=blocks, half=half, width=width)
    layer = (blocks, rows, width)
    cells = blocks * rows * width

    def out(*shape):
        return jax.ShapeDtypeStruct(shape, jnp.float32)

    def params(mib):
        return pltpu.CompilerParams(vmem_limit_bytes=mib << 20)

    def cost(ops):
        return pl.CostEstimate(flops=ops * cells, bytes_accessed=16 * cells, transcendentals=0)

    def scales(count):
        return [pltpu.VMEM((rows, width), jnp.float32), pltpu.VMEM((count, rows, width), jnp.float32)]

    def first(*fields):
        return pl.pallas_call(
            functools.partial(first_kernel, **sizes),
            out_shape=(out(2, *layer), out(2, blocks, half, width)),
            in_specs=[vmem] * 4,
            out_specs=(vmem,) * 2,
            scratch_shapes=scales(2),
            compiler_params=params(8),
            cost_estimate=cost(40),
            name="first",
        )(*fields)

    def early(*arrays):
        return pl.pallas_call(
            functools.partial(early_kernel, **sizes),
            out_shape=(out(2, *layer), out(2, *layer), out(blocks, half, width), out(blocks, half, width),
                       out(len(EARLY) * count, 8, 128)),
            in_specs=[vmem] * 7,
            out_specs=(vmem,) * 5,
            scratch_shapes=scales(4),
            compiler_params=params(12),
            cost_estimate=cost(400),
            name="early",
        )(*arrays)

    def late(*arrays):
        return pl.pallas_call(
            functools.partial(late_kernel, **sizes),
            out_shape=(out(*layer), out(2, *layer), out(8, moments * count)),
            in_specs=[vmem] * 14,
            out_specs=(vmem,) * 3,
            scratch_shapes=[
                pltpu.VMEM((3, *layer), jnp.float32),
                pltpu.VMEM((2, *layer), jnp.float32),
                pltpu.VMEM((4, *layer), jnp.float32),
                pltpu.VMEM((moments * count, 8, 128), jnp.float32),
                *scales(8),
            ],
            compiler_params=params(18),
            cost_estimate=cost(400),
            name="late",
        )(*arrays)

    return first, early, late


TERMS = (
    ((0, None), (1, None), (2, 0)), ((3, None), (4, 0), (2, 1)),
    ((5, None), (6, 0), (7, None)), ((8, None), (6, 1), (9, None)),
)


def combine_kernel(weights, *refs, blocks, half, width):
    arrays, (out, buffer, sems) = refs[:-3], refs[-3:]
    parity = lax.rem(lax.axis_index("gz"), 2)
    copies = []
    for n, (at_layer, at_half) in enumerate((
        (parity, parity), (1 - parity, parity), (1 - parity, 1 - parity), (parity, 1 - parity),
    )):
        terms = [arrays[ref] if at is None else arrays[ref].at[at] for ref, at in TERMS[n]]

        def tile(step, carry, terms=terms, n=n):
            at = pl.multiple_of(step * 8, 8)
            for c in range(width // 128):
                lanes = pl.ds(128 * c, 128)
                sums = [None] * blocks
                for k, term in enumerate(terms):
                    for v in range(blocks):
                        part = term[v, pl.ds(at, 8), lanes]
                        for w in range(blocks):
                            value = weights[k * blocks + v, w] * part
                            sums[w] = value if sums[w] is None else sums[w] + value
                for w in range(blocks):
                    buffer[n, w, pl.ds(at, 8), lanes] = sums[w]
            return carry

        lax.fori_loop(0, half // 8, tile, 0)
        copies.append(pltpu.make_async_copy(
            buffer.at[n],
            out.at[:, at_layer, pl.ds(pl.multiple_of(at_half * half, 8), half)],
            sems.at[n]))
        copies[-1].start()
    for copy in copies:
        copy.wait()


def combine(weights, arrays, blocks, half, width):
    vmem = pl.BlockSpec(memory_space=pltpu.VMEM)
    return pl.pallas_call(
        functools.partial(combine_kernel, blocks=blocks, half=half, width=width),
        out_shape=jax.ShapeDtypeStruct((blocks, 2, 2 * half, width), jnp.float32),
        in_specs=[pl.BlockSpec(memory_space=pltpu.SMEM)] + [vmem] * len(arrays),
        out_specs=pl.BlockSpec(memory_space=pl.ANY),
        scratch_shapes=[pltpu.VMEM((4, blocks, half, width), jnp.float32), pltpu.SemaphoreType.DMA((4,))],
        compiler_params=pltpu.CompilerParams(vmem_limit_bytes=12 << 20),
        name="combine",
    )(weights, *arrays)


def full_moments(nu, blocks):
    count = blocks * (blocks + 1) // 2
    pick = np.zeros((count, blocks * blocks), np.float32)
    n = 0
    for v in range(blocks):
        for w in range(v, blocks):
            pick[n, v * blocks + w] = pick[n, w * blocks + v] = 1.0
            n += 1
    full = jnp.dot(nu.reshape(-1, count), pick, precision=HIGHEST)
    return full.reshape(-1, blocks, blocks)


def dense(nu, blocks):
    b1, b2 = BETA[1], BETA[2]
    g02 = nu[2] - b1 * nu[0]
    g03 = nu[3] - b2 * nu[1]
    g13 = nu[4] + b1 * g02 - b2 * nu[2]
    gram = jnp.concatenate([
        jnp.concatenate([nu[0], nu[1], g02, g03], axis=1),
        jnp.concatenate([nu[1], nu[2], nu[3], g13], axis=1),
        jnp.concatenate([g02, nu[3], nu[4], nu[5]], axis=1),
        jnp.concatenate([g03, g13, nu[5], nu[6]], axis=1),
    ], axis=0)
    size = ITERS * blocks
    factor = jnp.linalg.cholesky(gram)
    inverse = jax.scipy.linalg.solve_triangular(
        factor[:size, :size], jnp.eye(size, dtype=jnp.float32), lower=True)
    flat = factor.reshape(ITERS + 1, blocks, size + blocks)
    shifted = [SPREAD * flat[k + 1] + CENTER * flat[k]
               + (SPREAD * BETA[k] * flat[k - 1] if BETA[k] else 0.0) for k in range(ITERS)]
    hessenberg = jnp.dot(inverse, jnp.concatenate(shifted, axis=0), precision=HIGHEST)
    row = lax.broadcasted_iota(jnp.int32, hessenberg.shape, 0) // blocks
    col = lax.broadcasted_iota(jnp.int32, hessenberg.shape, 1) // blocks
    hessenberg = jnp.where(col <= row + 1, hessenberg, 0.0)
    normal = jnp.dot(hessenberg, hessenberg.T, precision=HIGHEST)
    target = jnp.dot(hessenberg[:, :blocks], factor[:blocks, :blocks].T, precision=HIGHEST)
    coeffs = jax.scipy.linalg.cho_solve((jnp.linalg.cholesky(normal), True), target)
    weights = jnp.dot(inverse.T, coeffs, precision=HIGHEST)
    return hessenberg, weights


def body(right_side, diagonal):
    blocks, _, ny, width = right_side.shape
    half = ny // 2
    peers_z, peers_y = lax.axis_size("gz"), lax.axis_size("gy")
    even = lax.axis_index("gz") % 2 == 0
    field = jnp.concatenate([right_side, diagonal[None]], axis=0)
    above = lax.ppermute(field[:, :, ny - EDGE:], "gy", pairs(peers_y, 1))
    under = lax.ppermute(field[:, :, :EDGE], "gy", pairs(peers_y, -1))
    first = jnp.concatenate([field[:, :, :half + EDGE], above], axis=2)
    second = jnp.concatenate([field[:, :, half:], under, field[:, :, half - EDGE:half]], axis=2)

    swap = swap_pairs(peers_z, 1)
    inward = [(i, j) for i, j in pairs(peers_z, 2) if i % 2 == 0] + [(i, j) for i, j in pairs(peers_z, -2) if i % 2]
    outward = [(j, i) for i, j in inward]
    send_near = jnp.where(even, second[:, 1], first[:, 0])
    send_far = jnp.where(even, second[:, 0], first[:, 1])
    keep_near = jnp.where(even, first[:, 1], second[:, 0])
    keep_far = jnp.where(even, first[:, 0], second[:, 1])
    first_step, early, late = kernels(blocks, half, width)

    def move(array, links):
        return lax.ppermute(array, "gz", links)

    got_near = move(send_near, swap)
    in_one = move(keep_near[:blocks], inward)
    out_one = move(keep_far, outward)
    got_far = move(send_far, swap)
    out_two = move(keep_near, outward)
    in_two = move(got_near, inward)
    out_three = move(got_near[:blocks], outward)
    in_three = move(got_far, inward)
    mid1, sent1 = first_step(keep_near, got_near, got_far, out_one)
    back1 = move(sent1, swap)
    near1, near2, near_sent, far_sent, start = early(
        keep_far, keep_near, got_near, got_far, out_one, out_two, mid1)
    near_back2 = move(near_sent, swap)
    x1, x2, nu = late(
        in_one, in_two, in_three, keep_far, keep_near, got_near, got_far, out_one, out_two, out_three,
        mid1, near1, near2, start)
    nu = all_sum(nu[:1], ("gz", "gy"))
    nu, far_sent = lax.optimization_barrier((nu, far_sent))
    far_back2 = move(far_sent, swap)
    hessenberg, weights = dense(full_moments(nu, blocks), blocks)
    result = combine(
        weights,
        (keep_far, x1, x2, keep_near, near1, send_near, back1, near_back2, send_far, far_back2),
        blocks, half, width)
    return result, hessenberg


def solution(mesh):
    in_specs = (P(None, "gz", "gy", None), P("gz", "gy", None))
    out_specs = (P(None, "gz", "gy", None), P())

    return jax.shard_map(body, mesh=mesh, in_specs=in_specs, out_specs=out_specs, check_vma=False)
```

```python
import functools

import jax
import jax.numpy as jnp
import numpy as np
from jax import lax
from jax.experimental import pallas as pl
from jax.experimental.pallas import tpu as pltpu
from jax.sharding import PartitionSpec as P

ITERS = 3
EDGE = 4
CENTER, SPREAD = 7.6, 2.6
BETA = (0.0, 1.0, 1.5)
HIGHEST = lax.Precision.HIGHEST


def pairs(peers, step):
    return [(i, i + step) for i in range(peers) if 0 <= i + step < peers]


def swap_pairs(peers, bit):
    return [(i, i ^ bit) for i in range(peers)]


def all_parts(array, axes):
    peers = 1
    for axis in axes:
        peers *= lax.axis_size(axis)
    spread = jnp.broadcast_to(array[None], (peers, *array.shape))
    return lax.all_to_all(spread, axes, 0, 0)


def row_masks(half, width):
    rows = half + 2 * EDGE
    parity = lax.rem(lax.axis_index("gz"), 2)
    at_y = lax.axis_index("gy")
    no_below = jnp.logical_and(at_y == lax.axis_size("gy") - 1, parity == 1)
    no_above = jnp.logical_and(at_y == 0, parity == 0)
    row = lax.broadcasted_iota(jnp.int32, (rows, width), 0)
    below = jnp.where(no_below, 0.0, 1.0)
    above = jnp.where(no_above, 0.0, 1.0)
    return jnp.where(row < half, 1.0, jnp.where(row < half + EDGE, below, above))


def side_flags():
    place = lax.axis_index("gz")
    parity = lax.rem(place, 2)
    downward = jnp.where(place >= 2, 1.0, 0.0)
    upward = jnp.where(place < lax.axis_size("gz") - 2, 1.0, 0.0)
    return (jnp.where(parity == 0, downward, upward), jnp.where(parity == 0, upward, downward))


def set_scales(scale_ref, diag_ref, fields, blocks, slots, half, width):
    scale_ref[...] = row_masks(half, width) * (1.0 / SPREAD)
    low, high = side_flags()
    for slot, (layer, ref) in enumerate(zip(slots, fields)):
        value = scale_ref[...] * (ref[blocks] + (6.0 - CENTER))
        if layer < 4:
            value = value * low
        if layer > 7:
            value = value * high
        diag_ref[slot] = value


def step_of(scale, diag, low, mid, high, before, beta, flag=None):
    rows, width = mid.shape
    lane = lax.broadcasted_iota(jnp.int32, (rows, width), 1)
    beside = low + high
    beside = beside + pltpu.roll(mid, 1, 0) + pltpu.roll(mid, rows - 1, 0)
    beside = beside + jnp.where(lane == 0, 0.0, pltpu.roll(mid, 1, 1))
    beside = beside + jnp.where(lane == width - 1, 0.0, pltpu.roll(mid, width - 1, 1))
    if flag is not None:
        scale = scale * flag
    value = diag * mid - scale * beside
    if beta:
        value = value - beta * before
    return value


def gram_part(acc, views, moment, layers, blocks, half, width, start):
    left, right = views[moment // 2], views[(moment + 1) // 2]
    upper = [(v, w) for v in range(blocks) for w in range(v, blocks)]

    def spot(step, sums):
        at = pl.multiple_of(step * 8, 8)
        sums = list(sums)
        for layer in layers:
            for c in range(width // 128):
                lanes = pl.ds(128 * c, 128)
                rights = [right[layer][w, pl.ds(at, 8), lanes] for w in range(blocks)]
                for v in range(blocks):
                    one = rights[v] if left is right else left[layer][v, pl.ds(at, 8), lanes]
                    for n, (a, b) in enumerate(upper):
                        if a == v:
                            sums[n] = sums[n] + one * rights[b]
        return tuple(sums)

    zeros = tuple(jnp.zeros((8, 128), jnp.float32) for _ in upper)
    sums = lax.fori_loop(0, half // 8, spot, zeros)
    base = moment * len(upper)
    for n in range(len(upper)):
        acc[base + n] = sums[n] if start is None else sums[n] + start[base + n]


EARLY = {0: (7,), 1: (5, 6, 7), 2: (5, 6, 7), 3: (6, 7), 4: (6, 7)}
LATE = {1: (4,), 2: (4,), 3: (4, 5), 4: (4, 5), 5: (4, 5, 6, 7), 6: (4, 5, 6, 7)}


def first_kernel(*refs, blocks, half, width):
    fields = dict(zip((5, 6, 7, 8), refs[:4]))
    x1, sent, scale_ref, diag_ref = refs[4:]
    set_scales(scale_ref, diag_ref, [fields[n] for n in (6, 7)], blocks, (6, 7), half, width)

    def vector(v, carry):
        for slot, n in enumerate((6, 7)):
            value = step_of(
                scale_ref[...], diag_ref[slot], fields[n - 1][v], fields[n][v], fields[n + 1][v], None, 0.0)
            x1[slot, v] = value
            sent[slot, v] = value[:half]
        return carry

    lax.fori_loop(0, blocks, vector, 0)


def zero_kernel(*refs, blocks, half, width):
    fields = dict(zip((4, 5, 6), refs[:3]))
    gram_part(refs[3], (fields,), 0, (4, 5, 6), blocks, half, width, None)


def early_kernel(*refs, blocks, half, width):
    fields = dict(zip((4, 5, 6, 7, 8, 9), refs[:6]))
    before, start, x1, x2, near_sent, far_sent, acc, x1_out, scale_ref, diag_ref, sem = refs[6:]
    slots = (5, 6, 7, 8)
    set_scales(scale_ref, diag_ref, [fields[n] for n in slots], blocks, slots, half, width)
    flag = side_flags()[1]
    one = {5: x1.at[0], 6: before.at[0], 7: before.at[1], 8: x1.at[1]}

    def vector(v, carry):
        for n in (5, 8):
            one[n][v] = step_of(
                scale_ref[...], diag_ref[n - 5], fields[n - 1][v], fields[n][v], fields[n + 1][v],
                None, 0.0, flag if n == 8 else None)
        for slot, (n, sent) in enumerate(((6, near_sent), (7, far_sent))):
            value = step_of(
                scale_ref[...], diag_ref[n - 5], one[n - 1][v], one[n][v], one[n + 1][v],
                fields[n][v], BETA[1])
            x2[slot, v] = value
            sent[v] = value[:half]
        return carry

    lax.fori_loop(0, blocks, vector, 0)
    copy = pltpu.make_async_copy(x1.at[0, :, pl.ds(0, half)], x1_out, sem)
    copy.start()
    views = (fields, one, {n: x2.at[n - 6] for n in (6, 7)})
    for moment, layers in EARLY.items():
        gram_part(acc, views, moment, layers, blocks, half, width, start if moment == 0 else None)
    copy.wait()


def late_kernel(*refs, blocks, half, width):
    fields = dict(zip(range(1, 11), refs[:10]))
    mid1, near1, near2, start, x1_out, x2_out, nu_out, x1, x2, far1, far2, x3, acc, scale_ref, diag_ref, sems = refs[10:]
    slots = tuple(range(2, 10))
    set_scales(scale_ref, diag_ref, [fields[n] for n in slots], blocks, slots, half, width)
    low, high = side_flags()
    one = {2: far1.at[0], 3: far1.at[1], 4: x1, 9: far1.at[2],
           5: near1.at[0], 6: mid1.at[0], 7: mid1.at[1], 8: near1.at[1]}
    two = {3: far2.at[0], 4: x2.at[0], 5: x2.at[1], 6: near2.at[0], 7: near2.at[1], 8: far2.at[1]}
    three = {n: x3.at[n - 4] for n in (4, 5, 6, 7)}

    def flag_of(n):
        return low if n < 4 else high if n > 7 else None

    def vector(v, carry):
        for n in (2, 3, 4, 9):
            one[n][v] = step_of(
                scale_ref[...], diag_ref[n - 2], fields[n - 1][v], fields[n][v], fields[n + 1][v],
                None, 0.0, flag_of(n))
        for n in (3, 4, 5, 8):
            two[n][v] = step_of(
                scale_ref[...], diag_ref[n - 2], one[n - 1][v], one[n][v], one[n + 1][v],
                fields[n][v], BETA[1], flag_of(n))
        for n in (4, 5, 6, 7):
            three[n][v] = step_of(
                scale_ref[...], diag_ref[n - 2], two[n - 1][v], two[n][v], two[n + 1][v],
                one[n][v], BETA[2])
        return carry

    lax.fori_loop(0, blocks, vector, 0)
    copies = [pltpu.make_async_copy(x1.at[:, pl.ds(0, half)], x1_out, sems.at[0]),
              pltpu.make_async_copy(x2.at[:, :, pl.ds(0, half)], x2_out, sems.at[1])]
    for copy in copies:
        copy.start()
    views = (fields, one, two, three)
    upper = [(v, w) for v in range(blocks) for w in range(v, blocks)]
    acc[pl.ds(0, len(upper))] = start[pl.ds(0, len(upper))]
    for moment, layers in LATE.items():
        gram_part(acc, views, moment, layers, blocks, half, width, start if moment in EARLY else None)
    total = jnp.sum(acc[...], axis=1)
    nu_out[...] = lax.dot_general(
        jnp.ones((8, 128), jnp.float32), total, (((1,), (1,)), ((), ())),
        precision=HIGHEST, preferred_element_type=jnp.float32)
    for copy in copies:
        copy.wait()


def kernels(blocks, half, width):
    rows = half + 2 * EDGE
    moments = 2 * ITERS + 1
    count = blocks * (blocks + 1) // 2
    vmem = pl.BlockSpec(memory_space=pltpu.VMEM)
    hbm = pl.BlockSpec(memory_space=pl.ANY)
    sizes = dict(blocks=blocks, half=half, width=width)
    layer = (blocks, rows, width)
    cells = blocks * rows * width

    def out(*shape):
        return jax.ShapeDtypeStruct(shape, jnp.float32)

    def params(mib):
        return pltpu.CompilerParams(vmem_limit_bytes=mib << 20)

    def cost(ops):
        return pl.CostEstimate(flops=ops * cells, bytes_accessed=16 * cells, transcendentals=0)

    def scales(count):
        return [pltpu.VMEM((rows, width), jnp.float32), pltpu.VMEM((count, rows, width), jnp.float32)]

    def first(*fields):
        return pl.pallas_call(
            functools.partial(first_kernel, **sizes),
            out_shape=(out(2, *layer), out(2, blocks, half, width)),
            in_specs=[vmem] * 4,
            out_specs=(vmem,) * 2,
            scratch_shapes=scales(2),
            compiler_params=params(8),
            cost_estimate=cost(40),
            name="first",
        )(*fields)

    def zero(*fields):
        return pl.pallas_call(
            functools.partial(zero_kernel, **sizes),
            out_shape=out(count, 8, 128),
            in_specs=[vmem] * 3,
            out_specs=vmem,
            compiler_params=params(4),
            cost_estimate=cost(40),
            name="zero",
        )(*fields)

    def early(*arrays):
        return pl.pallas_call(
            functools.partial(early_kernel, **sizes),
            out_shape=(out(2, *layer), out(2, *layer), out(blocks, half, width), out(blocks, half, width),
                       out(len(EARLY) * count, 8, 128), out(blocks, half, width)),
            in_specs=[vmem] * 8,
            out_specs=(vmem,) * 5 + (hbm,),
            scratch_shapes=scales(4) + [pltpu.SemaphoreType.DMA],
            compiler_params=params(12),
            cost_estimate=cost(400),
            name="early",
        )(*arrays)

    def late(*arrays):
        return pl.pallas_call(
            functools.partial(late_kernel, **sizes),
            out_shape=(out(blocks, half, width), out(2, blocks, half, width), out(8, moments * count)),
            in_specs=[vmem] * 14,
            out_specs=(hbm, hbm, vmem),
            scratch_shapes=[
                pltpu.VMEM(layer, jnp.float32),
                pltpu.VMEM((2, *layer), jnp.float32),
                pltpu.VMEM((3, *layer), jnp.float32),
                pltpu.VMEM((2, *layer), jnp.float32),
                pltpu.VMEM((4, *layer), jnp.float32),
                pltpu.VMEM((moments * count, 8, 128), jnp.float32),
                *scales(8),
                pltpu.SemaphoreType.DMA((2,)),
            ],
            compiler_params=params(20),
            cost_estimate=cost(400),
            name="late",
        )(*arrays)

    return zero, first, early, late


def moment_tables(blocks):
    b1, b2 = BETA[1], BETA[2]
    size = 2 * ITERS + 1
    unit = np.eye(size)
    g02 = unit[2] - b1 * unit[0]
    g03 = unit[3] - b2 * unit[1]
    g13 = unit[4] + b1 * g02 - b2 * unit[2]
    table = [[unit[0], unit[1], g02, g03], [unit[1], unit[2], unit[3], g13],
             [g02, unit[3], unit[4], unit[5]], [g03, g13, unit[5], unit[6]]]
    pairs_of = [(m, v, w) for m in range(size) for v in range(blocks) for w in range(v, blocks)]
    rows = np.zeros((2, blocks, len(pairs_of)), np.float32)
    cols = np.zeros((2, len(pairs_of), ITERS + 1, ITERS + 1, blocks), np.float32)
    for n, (m, v, w) in enumerate(pairs_of):
        rows[0, v, n] = 1.0
        rows[1, w, n] = float(v != w)
        for i in range(ITERS + 1):
            for j in range(ITERS + 1):
                cols[0, n, i, j, w] = table[i][j][m]
                cols[1, n, i, j, v] = table[i][j][m]
    return rows, cols.reshape(2, len(pairs_of), -1)


def shift_table(blocks):
    table = np.zeros((ITERS, ITERS + 1))
    for k in range(ITERS):
        table[k, k + 1] = SPREAD
        table[k, k] = CENTER
        if k:
            table[k, k - 1] = SPREAD * BETA[k]
    return np.kron(table, np.eye(blocks)).astype(np.float32)


def contract(left, right, at_left, at_right):
    return lax.dot_general(left, right, (((at_left,), (at_right,)), ((), ())),
                           precision=HIGHEST, preferred_element_type=jnp.float32)


def solve_small(parts, rows, cols, shift, blocks):
    nu = jnp.sum(parts, axis=0)
    wide = contract(rows[0] * nu, cols[0], 1, 0) + contract(rows[1] * nu, cols[1], 1, 0)
    total, size = (ITERS + 1) * blocks, ITERS * blocks
    gram = jnp.concatenate([wide[:, total * i:total * i + total] for i in range(ITERS + 1)], axis=0)
    row = lax.broadcasted_iota(jnp.int32, (total, total), 0)
    col = lax.broadcasted_iota(jnp.int32, (total, total), 1)
    eye = jnp.where(row == col, 1.0, 0.0)
    both = jnp.concatenate([gram, eye], axis=1)
    below = lax.broadcasted_iota(jnp.int32, both.shape, 0)
    for j in range(total - 1):
        factor = both[:, j:j + 1] / both[j:j + 1, j:j + 1]
        both = both - jnp.where(below > j, factor, 0.0) * both[j:j + 1]
    pivots = jnp.sum(both[:, :total] * eye, axis=1, keepdims=True)
    both = both / jnp.sqrt(pivots)
    upper = jnp.where(row <= col, both[:, :total], 0.0)
    inverse = both[:size, total:total + size]
    hessenberg = contract(inverse, contract(shift, upper, 1, 1), 1, 0)
    row = lax.broadcasted_iota(jnp.int32, hessenberg.shape, 0) // blocks
    col = lax.broadcasted_iota(jnp.int32, hessenberg.shape, 1) // blocks
    hessenberg = jnp.where(col <= row + 1, hessenberg, 0.0)
    normal = contract(hessenberg, hessenberg, 1, 1)
    target = contract(hessenberg[:, :blocks], upper[:blocks, :blocks], 1, 0)
    both = jnp.concatenate([normal, target], axis=1)
    here = lax.broadcasted_iota(jnp.int32, both.shape, 0)
    for j in range(size):
        pivot = both[j:j + 1] / both[j:j + 1, j:j + 1]
        both = jnp.where(here == j, pivot, both - both[:, j:j + 1] * pivot)
    return hessenberg, contract(inverse.T, both[:, size:], 1, 0)


def blend(buffer, terms, splat, blocks, half, width):
    def tile(step, carry):
        at = pl.multiple_of(step * 8, 8)
        parts = [pl.ds(128 * c, 128) for c in range(width // 128)]
        sums = [[None] * len(parts) for _ in range(blocks)]
        for k, term in enumerate(terms):
            for v in range(blocks):
                values = [term[v, pl.ds(at, 8), lanes] for lanes in parts]
                for w in range(blocks):
                    scale = jnp.broadcast_to(splat[w, pl.ds(k * blocks + v, 1), :], (8, 128))
                    for c, value in enumerate(values):
                        value = scale * value
                        sums[w][c] = value if sums[w][c] is None else sums[w][c] + value
        for w in range(blocks):
            for c, lanes in enumerate(parts):
                buffer[w, pl.ds(at, 8), lanes] = sums[w][c]
        return carry

    lax.fori_loop(0, half // 8, tile, 0)


def place_of(n, half):
    parity = lax.rem(lax.axis_index("gz"), 2)
    layer = (parity, 1 - parity, 1 - parity, parity)[n]
    rows = (parity, parity, 1 - parity, 1 - parity)[n]
    return layer, pl.ds(pl.multiple_of(rows * half, 8), half)


TERMS = (((0, None), (1, None), (2, 0)), ((3, None), (4, None), (2, 1)), ((5, None), (6, 0), (7, None)))


def finish_kernel(parts, rows, cols, shift, *refs, blocks, half, width):
    arrays, (hess_out, splat, out, source, buffer, sems, out_sems) = refs[:8], refs[8:]
    copies = []
    for n, terms in enumerate(TERMS):
        for k, (ref, at) in enumerate(terms):
            ref = arrays[ref] if at is None else arrays[ref].at[at]
            copy = pltpu.make_async_copy(
                ref.at[pl.ds(0, blocks), pl.ds(0, half)], source.at[n, k], sems.at[n, k])
            copy.start()
            copies.append(copy)
    hessenberg, weights = solve_small(parts[...], rows, cols, shift[...], blocks)
    hess_out[...] = hessenberg
    for w in range(blocks):
        splat[w] = jnp.broadcast_to(weights[:, w:w + 1], (ITERS * blocks, 128))
    for copy in copies:
        copy.wait()
    sends = []
    for n in range(len(TERMS)):
        blend(buffer.at[n], [source.at[n, k] for k in range(ITERS)], splat, blocks, half, width)
        layer, at = place_of(n, half)
        sends.append(pltpu.make_async_copy(buffer.at[n], out.at[:, layer, at], out_sems.at[n]))
        sends[-1].start()
    for send in sends:
        send.wait()


def last_kernel(splat, field, one, two, _, out, buffer, sem, *, blocks, half, width):
    blend(buffer, [field, one.at[1], two], splat, blocks, half, width)
    layer, at = place_of(len(TERMS), half)
    send = pltpu.make_async_copy(buffer, out.at[:, layer, at], sem)
    send.start()
    send.wait()


def finish(parts, arrays, blocks, half, width):
    vmem = pl.BlockSpec(memory_space=pltpu.VMEM)
    hbm = pl.BlockSpec(memory_space=pl.ANY)
    rows, cols = moment_tables(blocks)
    size = ITERS * blocks
    piece = (blocks, half, width)
    return pl.pallas_call(
        functools.partial(finish_kernel, blocks=blocks, half=half, width=width),
        out_shape=(
            jax.ShapeDtypeStruct((size, size + blocks), jnp.float32),
            jax.ShapeDtypeStruct((blocks, size, 128), jnp.float32),
            jax.ShapeDtypeStruct((blocks, 2, 2 * half, width), jnp.float32),
        ),
        in_specs=[vmem] * 4 + [hbm] * len(arrays),
        out_specs=(vmem, vmem, hbm),
        scratch_shapes=[
            pltpu.VMEM((len(TERMS), ITERS, *piece), jnp.float32),
            pltpu.VMEM((len(TERMS), *piece), jnp.float32),
            pltpu.SemaphoreType.DMA((len(TERMS), ITERS)),
            pltpu.SemaphoreType.DMA((len(TERMS),)),
        ],
        compiler_params=pltpu.CompilerParams(vmem_limit_bytes=16 << 20),
        cost_estimate=pl.CostEstimate(flops=300 * blocks * half * width, bytes_accessed=1 << 23, transcendentals=0),
        name="finish",
    )(parts, rows, cols, shift_table(blocks), *arrays)


def last(splat, field, one, two, result, blocks, half, width):
    vmem = pl.BlockSpec(memory_space=pltpu.VMEM)
    hbm = pl.BlockSpec(memory_space=pl.ANY)
    return pl.pallas_call(
        functools.partial(last_kernel, blocks=blocks, half=half, width=width),
        out_shape=jax.ShapeDtypeStruct(result.shape, result.dtype),
        in_specs=[vmem] * 4 + [hbm],
        out_specs=hbm,
        scratch_shapes=[pltpu.VMEM((blocks, half, width), jnp.float32), pltpu.SemaphoreType.DMA],
        input_output_aliases={4: 0},
        compiler_params=pltpu.CompilerParams(vmem_limit_bytes=8 << 20),
        name="last",
    )(splat, field, one, two, result)


def body(right_side, diagonal):
    blocks, _, ny, width = right_side.shape
    half = ny // 2
    peers_z, peers_y = lax.axis_size("gz"), lax.axis_size("gy")
    even = lax.axis_index("gz") % 2 == 0
    field = jnp.concatenate([right_side, diagonal[None]], axis=0)
    above = lax.ppermute(field[:, :, ny - EDGE:], "gy", pairs(peers_y, 1))
    under = lax.ppermute(field[:, :, :EDGE], "gy", pairs(peers_y, -1))
    first = jnp.concatenate([field[:, :, :half + EDGE], above], axis=2)
    second = jnp.concatenate([field[:, :, half:], under, field[:, :, half - EDGE:half]], axis=2)

    swap = swap_pairs(peers_z, 1)
    inward = [(i, j) for i, j in pairs(peers_z, 2) if i % 2 == 0] + [(i, j) for i, j in pairs(peers_z, -2) if i % 2]
    outward = [(j, i) for i, j in inward]
    send_near = jnp.where(even, second[:, 1], first[:, 0])
    send_far = jnp.where(even, second[:, 0], first[:, 1])
    keep_near = jnp.where(even, first[:, 1], second[:, 0])
    keep_far = jnp.where(even, first[:, 0], second[:, 1])
    zero, first_step, early, late = kernels(blocks, half, width)

    def move(array, links):
        return lax.ppermute(array, "gz", links)

    got_near = move(send_near, swap)
    in_one = move(keep_near[:blocks], inward)
    out_one = move(keep_far, outward)
    got_far = move(send_far, swap)
    out_two = move(keep_near, outward)
    in_two = move(got_near, inward)
    out_three = move(got_near[:blocks], outward)
    in_three = move(got_far, inward)
    nu_zero = zero(keep_far, keep_near, got_near)
    mid1, sent1 = first_step(keep_near, got_near, got_far, out_one)
    back1 = move(sent1, swap)
    near1, near2, near_sent, far_sent, start, x1_near = early(
        keep_far, keep_near, got_near, got_far, out_one, out_two, mid1, nu_zero)
    near_back2 = move(near_sent, swap)
    x1_far, x2, nu = late(
        in_one, in_two, in_three, keep_far, keep_near, got_near, got_far, out_one, out_two, out_three,
        mid1, near1, near2, start)
    parts = all_parts(nu[:1], ("gz", "gy"))
    parts, far_sent = lax.optimization_barrier((parts, far_sent))
    far_back2 = move(far_sent, swap)
    hessenberg, splat, result = finish(
        parts, (keep_far, x1_far, x2, keep_near, x1_near, send_near, back1, near_back2),
        blocks, half, width)
    return last(splat, send_far, back1, far_back2, result, blocks, half, width), hessenberg


def solution(mesh):
    in_specs = (P(None, "gz", "gy", None), P("gz", "gy", None))
    out_specs = (P(None, "gz", "gy", None), P())

    return jax.shard_map(body, mesh=mesh, in_specs=in_specs, out_specs=out_specs, check_vma=False)
```

```python
import functools

import jax
import jax.numpy as jnp
import numpy as np
from jax import lax
from jax.experimental import pallas as pl
from jax.experimental.pallas import tpu as pltpu
from jax.sharding import PartitionSpec as P

BLK = 8
ITERS = 3
EDGE = 4
CENTER, SPREAD = 7.6, 2.6
BETA = (0.0, 1.0, 1.5)
HIGHEST = lax.Precision.HIGHEST


def pairs(peers, step):
    return [(i, i + step) for i in range(peers) if 0 <= i + step < peers]


def swap_pairs(peers, bit):
    return [(i, i ^ bit) for i in range(peers)]


def row_masks(half, width):
    rows = half + 2 * EDGE
    parity = lax.rem(lax.axis_index("gz"), 2)
    at_y = lax.axis_index("gy")
    no_below = jnp.logical_and(at_y == lax.axis_size("gy") - 1, parity == 1)
    no_above = jnp.logical_and(at_y == 0, parity == 0)
    row = lax.broadcasted_iota(jnp.int32, (rows, width), 0)
    below = jnp.where(no_below, 0.0, 1.0)
    above = jnp.where(no_above, 0.0, 1.0)
    return jnp.where(row < half, 1.0, jnp.where(row < half + EDGE, below, above))


def side_flags():
    place = lax.axis_index("gz")
    parity = lax.rem(place, 2)
    downward = jnp.where(place >= 2, 1.0, 0.0)
    upward = jnp.where(place < lax.axis_size("gz") - 2, 1.0, 0.0)
    return (jnp.where(parity == 0, downward, upward), jnp.where(parity == 0, upward, downward))


def pick(view, part, i):
    return view[part][i] if isinstance(view, tuple) else view[i + part * (BLK // 2)]


def entry(view, v, rows, lanes):
    half = BLK // 2
    return view[v // half][v % half, rows, lanes] if isinstance(view, tuple) else view[v, rows, lanes]


def diag_of(view):
    return view[0][BLK // 2] if isinstance(view, tuple) else view[BLK]


def set_scales(scale_ref, diag_ref, fields, slots, half, width):
    scale_ref[...] = row_masks(half, width) * (1.0 / SPREAD)
    low, high = side_flags()
    for slot, layer in enumerate(slots):
        value = scale_ref[...] * (diag_of(fields[layer]) + (6.0 - CENTER))
        if layer < 4:
            value = value * low
        if layer > 7:
            value = value * high
        diag_ref[slot] = value


def step_of(scale, diag, low, mid, high, before, beta, flag=None, count=None):
    rows, width = mid.shape
    count = count or rows
    own = mid[:count]
    lane = lax.broadcasted_iota(jnp.int32, (count, width), 1)
    beside = low[:count] + high[:count]
    beside = beside + pltpu.roll(mid, 1, 0)[:count] + pltpu.roll(mid, rows - 1, 0)[:count]
    beside = beside + jnp.where(lane == 0, 0.0, pltpu.roll(own, 1, 1))
    beside = beside + jnp.where(lane == width - 1, 0.0, pltpu.roll(own, width - 1, 1))
    scale = scale[:count]
    if flag is not None:
        scale = scale * flag
    value = diag[:count] * own - scale * beside
    if beta:
        value = value - beta * before[:count]
    return value


def gram_part(acc, views, moment, layers, blocks, half, width, start):
    left, right = views[moment // 2], views[(moment + 1) // 2]
    upper = [(v, w) for v in range(blocks) for w in range(v, blocks)]

    def spot(step, sums):
        at = pl.ds(pl.multiple_of(step * 8, 8), 8)
        sums = list(sums)
        for layer in layers:
            for c in range(width // 128):
                lanes = pl.ds(128 * c, 128)
                rights = [entry(right[layer], w, at, lanes) for w in range(blocks)]
                for v in range(blocks):
                    one = rights[v] if left is right else entry(left[layer], v, at, lanes)
                    for n, (a, b) in enumerate(upper):
                        if a == v:
                            sums[n] = sums[n] + one * rights[b]
        return tuple(sums)

    zeros = tuple(jnp.zeros((8, 128), jnp.float32) for _ in upper)
    sums = lax.fori_loop(0, half // 8, spot, zeros)
    base = moment * len(upper)
    for n in range(len(upper)):
        acc[base + n] = sums[n] if start is None else sums[n] + start[base + n]


def half_loop(body):
    lax.fori_loop(0, BLK // 2, lambda i, carry: (body(i), carry)[1], 0)


EARLY = {0: (7,), 1: (5, 6, 7), 2: (5, 6, 7), 3: (6, 7), 4: (6, 7)}
LATE = {1: (4,), 2: (4,), 3: (4, 5), 4: (4, 5), 5: (4, 5, 6, 7), 6: (4, 5, 6, 7)}


def first_kernel(*refs, part, blocks, half, width):
    near, mid, far_one, far_two, out_one, x1, sent, scale_ref, diag_ref, sem = refs
    fields = {5: near, 6: mid, 7: (far_one, far_two), 8: out_one}
    set_scales(scale_ref, diag_ref, fields, (6, 7), half, width)

    def vector(i):
        for slot, n in enumerate((6, 7)):
            x1[slot, i] = step_of(
                scale_ref[...], diag_ref[slot], *[pick(fields[m], part, i) for m in (n - 1, n, n + 1)], None, 0.0)

    half_loop(vector)
    copy = pltpu.make_async_copy(x1.at[:, :, pl.ds(0, half)], sent, sem)
    copy.start()
    copy.wait()


def zero_kernel(*refs, layers, add, blocks, half, width):
    fields = dict(zip(layers, refs))
    gram_part(refs[-1], (fields,), 0, layers, blocks, half, width, refs[len(layers)] if add else None)


def early_kernel(*refs, blocks, half, width):
    (keep_far, keep_near, got_near, far_one, far_two, out_one, out_two, mid_one, mid_two, start,
     x1, x2, near_sent, far_sent, acc, x1_out, scale_ref, diag_ref, sems) = refs
    fields = {4: keep_far, 5: keep_near, 6: got_near, 7: (far_one, far_two), 8: out_one, 9: out_two}
    slots = (5, 6, 7, 8)
    set_scales(scale_ref, diag_ref, fields, slots, half, width)
    flag = side_flags()[1]
    one = {5: x1.at[0], 6: (mid_one.at[0], mid_two.at[0]), 7: (mid_one.at[1], mid_two.at[1]), 8: x1.at[1]}

    def vector(i):
        for part in range(2):
            v = i + part * (BLK // 2)
            for n in (5, 8):
                one[n][v] = step_of(
                    scale_ref[...], diag_ref[n - 5], *[pick(fields[m], part, i) for m in (n - 1, n, n + 1)],
                    None, 0.0, flag if n == 8 else None)
            for slot, n in enumerate((6, 7)):
                x2[slot, v] = step_of(
                    scale_ref[...], diag_ref[n - 5], *[pick(one[m], part, i) for m in (n - 1, n, n + 1)],
                    pick(fields[n], part, i), BETA[1])

    half_loop(vector)
    copies = [pltpu.make_async_copy(ref.at[:, pl.ds(0, half)], out, sems.at[n]) for n, (ref, out) in enumerate(
        ((x2.at[0], near_sent), (x2.at[1], far_sent), (x1.at[0], x1_out)))]
    for copy in copies:
        copy.start()
    views = (fields, one, {n: x2.at[n - 6] for n in (6, 7)})
    for moment, layers in EARLY.items():
        gram_part(acc, views, moment, layers, blocks, half, width, start if moment == 0 else None)
    for copy in copies:
        copy.wait()


def late_kernel(*refs, part, blocks, half, width):
    (in_one, in_two, in_three, keep_far, keep_near, got_near, far_one, far_two, out_one, out_two, out_three,
     mid_one, mid_two, near1, near2) = refs[:15]
    rest = refs[15:]
    if part == 0:
        x1, x2, x3, far1, far2, scale_ref, diag_ref = rest
        third = (in_three,)
    else:
        (before, x1_first, x2_first, x3_first, start, x1_out, x2_out, nu_out,
         x1, x2, x3, far1, far2, acc, scale_ref, diag_ref, sems) = rest
        third = (before, in_three)
    third = third + (None,) * (2 - len(third))
    fields = {1: in_one, 2: in_two, 3: third, 4: keep_far, 5: keep_near, 6: got_near, 7: (far_one, far_two),
              8: out_one, 9: out_two, 10: (out_three, out_three)}
    slots = tuple(range(2, 10))
    set_scales(scale_ref, diag_ref, fields, slots, half, width)
    low, high = side_flags()
    mine = {2: far1.at[0], 3: far1.at[1], 4: x1, 9: far1.at[2]}
    one = {5: near1.at[0], 8: near1.at[1], 6: (mid_one.at[0], mid_two.at[0]), 7: (mid_one.at[1], mid_two.at[1]),
           **{n: (ref, ref) for n, ref in mine.items()}}
    mine_two = {3: far2.at[0], 4: x2.at[0], 5: x2.at[1], 8: far2.at[1]}
    two = {6: near2.at[0], 7: near2.at[1], **{n: (ref, ref) for n, ref in mine_two.items()}}

    def flag_of(n):
        return low if n < 4 else high if n > 7 else None

    def vector(i):
        for n, count in ((2, half), (3, None), (4, None), (9, half)):
            value = step_of(
                scale_ref[...], diag_ref[n - 2], *[pick(fields[m], part, i) for m in (n - 1, n, n + 1)],
                None, 0.0, flag_of(n), count)
            mine[n][i, pl.ds(0, value.shape[0])] = value
        for n, count in ((3, half), (4, None), (5, None), (8, half)):
            value = step_of(
                scale_ref[...], diag_ref[n - 2], *[pick(one[m], part, i) for m in (n - 1, n, n + 1)],
                pick(fields[n], part, i), BETA[1], flag_of(n), count)
            mine_two[n][i, pl.ds(0, value.shape[0])] = value
        for n in (4, 5, 6, 7):
            x3[n - 4, i] = step_of(
                scale_ref[...], diag_ref[n - 2], *[pick(two[m], part, i) for m in (n - 1, n, n + 1)],
                pick(one[n], part, i), BETA[2], None, half)

    half_loop(vector)
    if part == 0:
        return
    copies = []
    for n, (x1_half, x2_half) in enumerate(((x1_first, x2_first), (x1, x2))):
        vectors = pl.ds(n * (BLK // 2), BLK // 2)
        copies.append(pltpu.make_async_copy(x1_half.at[:, pl.ds(0, half)], x1_out.at[vectors], sems.at[2 * n]))
        copies.append(pltpu.make_async_copy(
            x2_half.at[:, :, pl.ds(0, half)], x2_out.at[:, vectors], sems.at[2 * n + 1]))
    for copy in copies:
        copy.start()
    views = (fields, {**one, 4: (x1_first, x1)},
             {**two, 4: (x2_first.at[0], x2.at[0]), 5: (x2_first.at[1], x2.at[1])},
             {n: (x3_first.at[n - 4], x3.at[n - 4]) for n in (4, 5, 6, 7)})
    upper = blocks * (blocks + 1) // 2
    acc[pl.ds(0, upper)] = start[pl.ds(0, upper)]
    for moment, layers in LATE.items():
        gram_part(acc, views, moment, layers, blocks, half, width, start if moment in EARLY else None)
    total = jnp.sum(acc[...], axis=1)
    sums = lax.dot_general(
        jnp.ones((8, 128), jnp.float32), total, (((1,), (1,)), ((), ())),
        precision=HIGHEST, preferred_element_type=jnp.float32)
    nu_out[...] = jnp.broadcast_to(sums[:1][None], nu_out.shape)
    for copy in copies:
        copy.wait()


def kernels(blocks, half, width, peers):
    rows = half + 2 * EDGE
    moments = 2 * ITERS + 1
    count = blocks * (blocks + 1) // 2
    vmem = pl.BlockSpec(memory_space=pltpu.VMEM)
    hbm = pl.BlockSpec(memory_space=pltpu.HBM)
    sizes = dict(blocks=blocks, half=half, width=width)
    layer = (blocks, rows, width)
    part_layer = (blocks // 2, rows, width)
    cells = blocks * rows * width

    def out(*shape):
        return jax.ShapeDtypeStruct(shape, jnp.float32)

    def far(*shape):
        return pltpu.HBM(shape, jnp.float32)

    def scales(number):
        return [pltpu.VMEM((rows, width), jnp.float32), pltpu.VMEM((number, rows, width), jnp.float32)]

    def call(kernel, arrays, outs, scratch, mib, ops, **static):
        return pl.pallas_call(
            functools.partial(kernel, **sizes, **static),
            out_shape=outs,
            in_specs=[vmem] * len(arrays),
            out_specs=tuple(vmem if isinstance(o, jax.ShapeDtypeStruct) else hbm for o in outs),
            scratch_shapes=scratch,
            compiler_params=pltpu.CompilerParams(vmem_limit_bytes=mib << 20),
            cost_estimate=pl.CostEstimate(flops=ops * cells, bytes_accessed=16 * cells, transcendentals=0),
        )(*arrays)

    def zero(arrays, layers, add):
        return call(zero_kernel, arrays, (out(count, 8, 128),), [], 4, 20, layers=layers, add=add)[0]

    def first(arrays, part):
        return call(first_kernel, arrays, (out(2, *part_layer), far(2, blocks // 2, half, width)),
                    scales(2) + [pltpu.SemaphoreType.DMA], 8, 20, part=part)

    def early(*arrays):
        outs = (out(2, *layer), out(2, *layer), far(blocks, half, width), far(blocks, half, width),
                out(len(EARLY) * count, 8, 128), far(blocks, half, width))
        return call(early_kernel, arrays, outs, scales(4) + [pltpu.SemaphoreType.DMA((3,))], 12, 200)

    def late(arrays, part):
        mine = ((part_layer), (2, *part_layer), (4, blocks // 2, half, width))
        work = [pltpu.VMEM((3, *part_layer), jnp.float32), pltpu.VMEM((2, *part_layer), jnp.float32)]
        if part == 0:
            return call(late_kernel, arrays, tuple(out(*m) for m in mine), work + scales(8), 12, 100, part=0)
        outs = (far(blocks, half, width), far(2, blocks, half, width), out(peers, 1, moments * count))
        work = [pltpu.VMEM(m, jnp.float32) for m in mine] + work + [
            pltpu.VMEM((moments * count, 8, 128), jnp.float32), *scales(8), pltpu.SemaphoreType.DMA((4,))]
        return call(late_kernel, arrays, outs, work, 18, 200, part=1)

    return zero, first, early, late


def moment_tables(blocks):
    b1, b2 = BETA[1], BETA[2]
    size = 2 * ITERS + 1
    unit = np.eye(size)
    g02 = unit[2] - b1 * unit[0]
    g03 = unit[3] - b2 * unit[1]
    g13 = unit[4] + b1 * g02 - b2 * unit[2]
    table = [[unit[0], unit[1], g02, g03], [unit[1], unit[2], unit[3], g13],
             [g02, unit[3], unit[4], unit[5]], [g03, g13, unit[5], unit[6]]]
    pairs_of = [(m, v, w) for m in range(size) for v in range(blocks) for w in range(v, blocks)]
    rows = np.zeros((2, blocks, len(pairs_of)), np.float32)
    cols = np.zeros((2, len(pairs_of), ITERS + 1, ITERS + 1, blocks), np.float32)
    for n, (m, v, w) in enumerate(pairs_of):
        rows[0, v, n] = 1.0
        rows[1, w, n] = float(v != w)
        for i in range(ITERS + 1):
            for j in range(ITERS + 1):
                cols[0, n, i, j, w] = table[i][j][m]
                cols[1, n, i, j, v] = table[i][j][m]
    return rows, cols.reshape(2, len(pairs_of), -1)


def shift_table(blocks):
    table = np.zeros((ITERS, ITERS + 1))
    for k in range(ITERS):
        table[k, k + 1] = SPREAD
        table[k, k] = CENTER
        if k:
            table[k, k - 1] = SPREAD * BETA[k]
    return np.kron(table, np.eye(blocks)).astype(np.float32)


def contract(left, right, at_left, at_right):
    return lax.dot_general(left, right, (((at_left,), (at_right,)), ((), ())),
                           precision=HIGHEST, preferred_element_type=jnp.float32)


def solve_small(parts, rows, cols, shift, blocks):
    nu = jnp.sum(parts, axis=0)
    wide = sum(contract(rows[n] * nu, cols[n].astype(jnp.float32), 1, 0) for n in range(2))
    total, size = (ITERS + 1) * blocks, ITERS * blocks
    gram = jnp.concatenate([wide[:, total * i:total * i + total] for i in range(ITERS + 1)], axis=0)
    row = lax.broadcasted_iota(jnp.int32, (total, total), 0)
    col = lax.broadcasted_iota(jnp.int32, (total, total), 1)
    eye = jnp.where(row == col, 1.0, 0.0)
    moved = contract(shift, gram, 1, 0)
    factors = jnp.concatenate([gram, eye], axis=1)
    solving = jnp.concatenate([contract(moved, shift, 1, 1), moved[:, :blocks]], axis=1)
    below = lax.broadcasted_iota(jnp.int32, factors.shape, 0)
    here = lax.broadcasted_iota(jnp.int32, solving.shape, 0)
    for j in range(total - 1):
        scale = factors[j:j + 1] / factors[j:j + 1, j:j + 1]
        factors = factors - jnp.where(below > j, factors[:, j:j + 1], 0.0) * scale
        if j < size:
            pivot = solving[j:j + 1] / solving[j:j + 1, j:j + 1]
            solving = jnp.where(here == j, pivot, solving - solving[:, j:j + 1] * pivot)
    pivots = jnp.sum(factors[:, :total] * eye, axis=1, keepdims=True)
    factors = factors / jnp.sqrt(pivots)
    upper = jnp.where(row <= col, factors[:, :total], 0.0)
    inverse = factors[:size, total:total + size]
    hessenberg = contract(inverse, contract(shift, upper, 1, 1), 1, 0)
    row = lax.broadcasted_iota(jnp.int32, hessenberg.shape, 0) // blocks
    col = lax.broadcasted_iota(jnp.int32, hessenberg.shape, 1) // blocks
    return jnp.where(col <= row + 1, hessenberg, 0.0), solving[:, size:]


def blend(buffer, terms, splat, blocks, half, width):
    def tile(step, carry):
        at = pl.multiple_of(step * 8, 8)
        parts = [pl.ds(128 * c, 128) for c in range(width // 128)]
        sums = [[None] * len(parts) for _ in range(blocks)]
        for k, term in enumerate(terms):
            for v in range(blocks):
                values = [term[v, pl.ds(at, 8), lanes] for lanes in parts]
                for w in range(blocks):
                    scale = jnp.broadcast_to(splat[w, pl.ds(k * blocks + v, 1), :], (8, 128))
                    for c, value in enumerate(values):
                        value = scale * value
                        sums[w][c] = value if sums[w][c] is None else sums[w][c] + value
        for w in range(blocks):
            for c, lanes in enumerate(parts):
                buffer[w, pl.ds(at, 8), lanes] = sums[w][c]
        return carry

    lax.fori_loop(0, half // 8, tile, 0)


def place_of(n, half):
    parity = lax.rem(lax.axis_index("gz"), 2)
    layer = (parity, 1 - parity, 1 - parity, parity)[n]
    rows = (parity, parity, 1 - parity, 1 - parity)[n]
    return layer, pl.ds(pl.multiple_of(rows * half, 8), half)


TERMS = (((0, None), (1, None), (2, 0)), ((3, None), (4, None), (2, 1)))


def finish_kernel(parts, rows, cols, shift, *refs, blocks, half, width):
    arrays, (hess_out, splat, out, source, buffer, sems, out_sems) = refs[:5], refs[5:]
    copies = []
    for n, terms in enumerate(TERMS):
        for k, (ref, at) in enumerate(terms):
            ref = arrays[ref] if at is None else arrays[ref].at[at]
            copy = pltpu.make_async_copy(
                ref.at[pl.ds(0, blocks), pl.ds(0, half)], source.at[n, k], sems.at[n, k])
            copy.start()
            copies.append(copy)
    hessenberg, weights = solve_small(parts[...], rows, cols, shift[...], blocks)
    hess_out[...] = hessenberg
    for w in range(blocks):
        splat[w] = jnp.broadcast_to(weights[:, w:w + 1], (ITERS * blocks, 128))
    for copy in copies:
        copy.wait()
    sends = []
    for n in range(len(TERMS)):
        blend(buffer.at[n], [source.at[n, k] for k in range(ITERS)], splat, blocks, half, width)
        layer, at = place_of(n, half)
        sends.append(pltpu.make_async_copy(buffer.at[n], out.at[:, layer, at], out_sems.at[n]))
        sends[-1].start()
    for send in sends:
        send.wait()


def others_kernel(splat, near0, far0, one_first, one_second, near2, far2, _, out, source, buffer, sems, out_sems, *,
                  blocks, half, width):
    loads = []
    for n, (zero, two) in enumerate(((near0, near2), (far0, far2))):
        for k, (term, at) in enumerate((
            (zero.at[pl.ds(0, blocks), pl.ds(0, half)], source.at[n, 0]),
            (one_first.at[n], source.at[n, 1, pl.ds(0, blocks // 2)]),
            (one_second.at[n], source.at[n, 1, pl.ds(blocks // 2, blocks // 2)]),
            (two, source.at[n, 2]),
        )):
            loads.append(pltpu.make_async_copy(term, at, sems.at[n, k]))
            loads[-1].start()
    sends = []
    for n in range(2):
        for load in loads[4 * n:4 * n + 4]:
            load.wait()
        blend(buffer.at[n], [source.at[n, k] for k in range(ITERS)], splat, blocks, half, width)
        layer, at = place_of(2 + n, half)
        sends.append(pltpu.make_async_copy(buffer.at[n], out.at[:, layer, at], out_sems.at[n]))
        sends[-1].start()
    for send in sends:
        send.wait()


def in_hbm(array):
    return pltpu.with_memory_space_constraint(array, pltpu.HBM)


def finish(parts, arrays, blocks, half, width):
    vmem = pl.BlockSpec(memory_space=pltpu.VMEM)
    hbm = pl.BlockSpec(memory_space=pltpu.HBM)
    rows, cols = moment_tables(blocks)
    size = ITERS * blocks
    piece = (blocks, half, width)
    return pl.pallas_call(
        functools.partial(finish_kernel, blocks=blocks, half=half, width=width),
        out_shape=(
            jax.ShapeDtypeStruct((size, size + blocks), jnp.float32),
            jax.ShapeDtypeStruct((blocks, size, 128), jnp.float32),
            jax.ShapeDtypeStruct((blocks, 2, 2 * half, width), jnp.float32),
        ),
        in_specs=[vmem] * 4 + [hbm] * len(arrays),
        out_specs=(vmem, vmem, hbm),
        scratch_shapes=[
            pltpu.VMEM((len(TERMS), ITERS, *piece), jnp.float32),
            pltpu.VMEM((len(TERMS), *piece), jnp.float32),
            pltpu.SemaphoreType.DMA((len(TERMS), ITERS)),
            pltpu.SemaphoreType.DMA((len(TERMS),)),
        ],
        compiler_params=pltpu.CompilerParams(vmem_limit_bytes=16 << 20),
        cost_estimate=pl.CostEstimate(flops=300 * blocks * half * width, bytes_accessed=1 << 23, transcendentals=0),
        name="finish",
    )(parts, rows, cols.astype(jnp.bfloat16), shift_table(blocks), *[in_hbm(array) for array in arrays])


def others(splat, near0, far0, one_first, one_second, near2, far2, result, half, width):
    vmem = pl.BlockSpec(memory_space=pltpu.VMEM)
    hbm = pl.BlockSpec(memory_space=pltpu.HBM)
    blocks = near2.shape[0]
    return pl.pallas_call(
        functools.partial(others_kernel, blocks=blocks, half=half, width=width),
        out_shape=jax.ShapeDtypeStruct(result.shape, result.dtype),
        in_specs=[vmem] + [hbm] * 2 + [pl.BlockSpec(memory_space=pl.ANY)] * 4 + [hbm],
        out_specs=hbm,
        scratch_shapes=[
            pltpu.VMEM((2, ITERS, blocks, half, width), jnp.float32),
            pltpu.VMEM((2, blocks, half, width), jnp.float32),
            pltpu.SemaphoreType.DMA((2, 4)),
            pltpu.SemaphoreType.DMA((2,)),
        ],
        input_output_aliases={7: 0},
        compiler_params=pltpu.CompilerParams(vmem_limit_bytes=8 << 20),
        name="others",
    )(splat, in_hbm(near0), in_hbm(far0), one_first, one_second, near2, far2, result)


def body(right_side, diagonal):
    blocks, _, ny, width = right_side.shape
    half = ny // 2
    peers_z, peers_y = lax.axis_size("gz"), lax.axis_size("gy")
    even = lax.axis_index("gz") % 2 == 0
    field = jnp.concatenate([right_side, diagonal[None]], axis=0)
    above = lax.ppermute(field[:, :, ny - EDGE:], "gy", pairs(peers_y, 1))
    under = lax.ppermute(field[:, :, :EDGE], "gy", pairs(peers_y, -1))
    first = jnp.concatenate([field[:, :, :half + EDGE], above], axis=2)
    second = jnp.concatenate([field[:, :, half:], under, field[:, :, half - EDGE:half]], axis=2)

    swap = swap_pairs(peers_z, 1)
    inward = [(i, j) for i, j in pairs(peers_z, 2) if i % 2 == 0] + [(i, j) for i, j in pairs(peers_z, -2) if i % 2]
    outward = [(j, i) for i, j in inward]
    send_near = jnp.where(even, second[:, 1], first[:, 0])
    send_far = jnp.where(even, second[:, 0], first[:, 1])
    keep_near = jnp.where(even, first[:, 1], second[:, 0])
    keep_far = jnp.where(even, first[:, 0], second[:, 1])
    zero, first_step, early, late = kernels(blocks, half, width, peers_z * peers_y)

    def move(array, links):
        return lax.ppermute(array, "gz", links)

    middle = blocks // 2
    got_near = move(send_near, swap)
    in_one = move(keep_near[:blocks, :half], inward)
    out_one = move(keep_far, outward)
    far_a = move(jnp.concatenate([send_far[:middle], send_far[blocks:]], axis=0), swap)
    far_b = move(send_far[middle:blocks], swap)
    out_two = move(keep_near, outward)
    in_two = move(got_near, inward)
    out_a = move(got_near[:middle, :half], outward)
    out_b = move(got_near[middle:blocks, :half], outward)
    nu_zero = zero((keep_far, keep_near), (4, 5), False)
    mid_a, sent_a = first_step((keep_near, got_near, far_a, far_a, out_one), 0)
    back_a = move(sent_a, swap)
    in_a = move(far_a, inward)
    nu_zero = zero((got_near, nu_zero), (6,), True)
    mid_b, sent_b = first_step((keep_near, got_near, far_a, far_b, out_one), 1)
    back_b = move(sent_b, swap)
    in_b = move(far_b, inward)
    near1, near2, near_sent, far_sent, start, x1_near = early(
        keep_far, keep_near, got_near, far_a, far_b, out_one, out_two, mid_a, mid_b, nu_zero)
    near_back2 = move(near_sent, swap)
    first_half = late((in_one, in_two, in_a, keep_far, keep_near, got_near, far_a, far_b, out_one, out_two,
                       out_a, mid_a, mid_b, near1, near2), 0)
    x1_far, x2, nu = late((in_one, in_two, in_b, keep_far, keep_near, got_near, far_a, far_b, out_one, out_two,
                           out_b, mid_a, mid_b, near1, near2, in_a, *first_half, start), 1)
    parts = lax.all_to_all(nu, ("gz", "gy"), 0, 0)
    far_back2 = move(far_sent, swap)
    hessenberg, splat, result = finish(
        parts, (keep_far, x1_far, x2, keep_near, x1_near), blocks, half, width)
    result = others(splat, send_near, send_far, back_a, back_b, near_back2, far_back2, result, half, width)
    return result, hessenberg


def solution(mesh):
    in_specs = (P(None, "gz", "gy", None), P("gz", "gy", None))
    out_specs = (P(None, "gz", "gy", None), P())

    return jax.shard_map(body, mesh=mesh, in_specs=in_specs, out_specs=out_specs, check_vma=False)
```

```python
import functools

import jax
import jax.numpy as jnp
import numpy as np
from jax import lax
from jax.experimental import pallas as pl
from jax.experimental.pallas import tpu as pltpu
from jax.sharding import PartitionSpec as P

BLK = 8
ITERS = 3
EDGE = 4
CENTER, SPREAD = 7.6, 2.6
BETA = (0.0, 1.0, 1.5)
HIGHEST = lax.Precision.HIGHEST


def pairs(peers, step):
    return [(i, i + step) for i in range(peers) if 0 <= i + step < peers]


def swap_pairs(peers, bit):
    return [(i, i ^ bit) for i in range(peers)]


def row_masks(half, width):
    rows = half + 2 * EDGE
    parity = lax.rem(lax.axis_index("gz"), 2)
    at_y = lax.axis_index("gy")
    no_below = jnp.logical_and(at_y == lax.axis_size("gy") - 1, parity == 1)
    no_above = jnp.logical_and(at_y == 0, parity == 0)
    row = lax.broadcasted_iota(jnp.int32, (rows, width), 0)
    below = jnp.where(no_below, 0.0, 1.0)
    above = jnp.where(no_above, 0.0, 1.0)
    return jnp.where(row < half, 1.0, jnp.where(row < half + EDGE, below, above))


def side_flags():
    place = lax.axis_index("gz")
    parity = lax.rem(place, 2)
    downward = jnp.where(place >= 2, 1.0, 0.0)
    upward = jnp.where(place < lax.axis_size("gz") - 2, 1.0, 0.0)
    return (jnp.where(parity == 0, downward, upward), jnp.where(parity == 0, upward, downward))


def pick(view, part, i):
    return view[part][i] if isinstance(view, tuple) else view[i + part * (BLK // 2)]


def entry(view, v, rows, lanes):
    half = BLK // 2
    return view[v // half][v % half, rows, lanes] if isinstance(view, tuple) else view[v, rows, lanes]


def diag_of(view):
    return view[0][BLK // 2] if isinstance(view, tuple) else view[BLK]


def set_scales(scale_ref, diag_ref, fields, slots, half, width, affine):
    center, inverse = (CENTER, 1.0 / SPREAD) if affine is None else (affine[0, 0], affine[0, 1])
    scale_ref[...] = row_masks(half, width) * inverse
    low, high = side_flags()
    for slot, layer in enumerate(slots):
        value = scale_ref[...] * (diag_of(fields[layer]) + (6.0 - center))
        if layer < 4:
            value = value * low
        if layer > 7:
            value = value * high
        diag_ref[slot] = value


def step_of(scale, diag, low, mid, high, before, beta, flag=None, count=None):
    rows, width = mid.shape
    count = count or rows
    own = mid[:count]
    lane = lax.broadcasted_iota(jnp.int32, (count, width), 1)
    beside = low[:count] + high[:count]
    beside = beside + pltpu.roll(mid, 1, 0)[:count] + pltpu.roll(mid, rows - 1, 0)[:count]
    beside = beside + jnp.where(lane == 0, 0.0, pltpu.roll(own, 1, 1))
    beside = beside + jnp.where(lane == width - 1, 0.0, pltpu.roll(own, width - 1, 1))
    scale = scale[:count]
    if flag is not None:
        scale = scale * flag
    value = diag[:count] * own - scale * beside
    if beta:
        value = value - beta * before[:count]
    return value


def gram_part(acc, views, moment, layers, blocks, half, width, start):
    left, right = views[moment // 2], views[(moment + 1) // 2]
    upper = [(v, w) for v in range(blocks) for w in range(v, blocks)]

    def spot(step, sums):
        at = pl.ds(pl.multiple_of(step * 8, 8), 8)
        sums = list(sums)
        for layer in layers:
            for c in range(width // 128):
                lanes = pl.ds(128 * c, 128)
                rights = [entry(right[layer], w, at, lanes) for w in range(blocks)]
                for v in range(blocks):
                    one = rights[v] if left is right else entry(left[layer], v, at, lanes)
                    for n, (a, b) in enumerate(upper):
                        if a == v:
                            sums[n] = sums[n] + one * rights[b]
        return tuple(sums)

    zeros = tuple(jnp.zeros((8, 128), jnp.float32) for _ in upper)
    sums = lax.fori_loop(0, half // 8, spot, zeros)
    base = moment * len(upper)
    for n in range(len(upper)):
        acc[base + n] = sums[n] if start is None else sums[n] + start[base + n]


def half_loop(body):
    lax.fori_loop(0, BLK // 2, lambda i, carry: (body(i), carry)[1], 0)


EARLY = {0: (7,), 1: (5, 6, 7), 2: (5, 6, 7), 3: (6, 7), 4: (6, 7)}
LATE = {1: (4,), 2: (4,), 3: (4, 5), 4: (4, 5), 5: (4, 5, 6, 7), 6: (4, 5, 6, 7)}


def first_kernel(*refs, affine, part, blocks, half, width):
    near, mid, far_one, far_two, out_one, x1, sent, scale_ref, diag_ref, sem = refs
    fields = {5: near, 6: mid, 7: (far_one, far_two), 8: out_one}
    set_scales(scale_ref, diag_ref, fields, (6, 7), half, width, affine)

    def vector(i):
        for slot, n in enumerate((6, 7)):
            x1[slot, i] = step_of(
                scale_ref[...], diag_ref[slot], *[pick(fields[m], part, i) for m in (n - 1, n, n + 1)], None, 0.0)

    half_loop(vector)
    copy = pltpu.make_async_copy(x1.at[:, :, pl.ds(0, half)], sent, sem)
    copy.start()
    copy.wait()


def zero_kernel(*refs, affine, layers, add, blocks, half, width):
    fields = dict(zip(layers, refs))
    gram_part(refs[-1], (fields,), 0, layers, blocks, half, width, refs[len(layers)] if add else None)


def early_kernel(*refs, affine, blocks, half, width):
    (keep_far, keep_near, got_near, far_one, far_two, out_one, out_two, mid_one, mid_two, start,
     x1, x2, near_sent, far_sent, acc, x1_out, scale_ref, diag_ref, sems) = refs
    fields = {4: keep_far, 5: keep_near, 6: got_near, 7: (far_one, far_two), 8: out_one, 9: out_two}
    slots = (5, 6, 7, 8)
    set_scales(scale_ref, diag_ref, fields, slots, half, width, affine)
    flag = side_flags()[1]
    one = {5: x1.at[0], 6: (mid_one.at[0], mid_two.at[0]), 7: (mid_one.at[1], mid_two.at[1]), 8: x1.at[1]}

    def vector(i):
        for part in range(2):
            v = i + part * (BLK // 2)
            for n in (5, 8):
                one[n][v] = step_of(
                    scale_ref[...], diag_ref[n - 5], *[pick(fields[m], part, i) for m in (n - 1, n, n + 1)],
                    None, 0.0, flag if n == 8 else None)
            for slot, n in enumerate((6, 7)):
                x2[slot, v] = step_of(
                    scale_ref[...], diag_ref[n - 5], *[pick(one[m], part, i) for m in (n - 1, n, n + 1)],
                    pick(fields[n], part, i), BETA[1])

    half_loop(vector)
    copies = [pltpu.make_async_copy(ref.at[:, pl.ds(0, half)], out, sems.at[n]) for n, (ref, out) in enumerate(
        ((x2.at[0], near_sent), (x2.at[1], far_sent), (x1.at[0], x1_out)))]
    for copy in copies:
        copy.start()
    views = (fields, one, {n: x2.at[n - 6] for n in (6, 7)})
    for moment, layers in EARLY.items():
        gram_part(acc, views, moment, layers, blocks, half, width, start if moment == 0 else None)
    for copy in copies:
        copy.wait()


def late_kernel(*refs, affine, part, blocks, half, width):
    (in_one, in_two, in_three, keep_far, keep_near, got_near, far_one, far_two, out_one, out_two, out_three,
     mid_one, mid_two, near1, near2) = refs[:15]
    rest = refs[15:]
    if part == 0:
        x1, x2, x3, far1, far2, scale_ref, diag_ref = rest
        third = (in_three,)
    else:
        (before, x1_first, x2_first, x3_first, start, x1_out, x2_out, nu_out,
         x1, x2, x3, far1, far2, acc, scale_ref, diag_ref, sems) = rest
        third = (before, in_three)
    third = third + (None,) * (2 - len(third))
    fields = {1: in_one, 2: in_two, 3: third, 4: keep_far, 5: keep_near, 6: got_near, 7: (far_one, far_two),
              8: out_one, 9: out_two, 10: (out_three, out_three)}
    slots = tuple(range(2, 10))
    set_scales(scale_ref, diag_ref, fields, slots, half, width, affine)
    low, high = side_flags()
    mine = {2: far1.at[0], 3: far1.at[1], 4: x1, 9: far1.at[2]}
    one = {5: near1.at[0], 8: near1.at[1], 6: (mid_one.at[0], mid_two.at[0]), 7: (mid_one.at[1], mid_two.at[1]),
           **{n: (ref, ref) for n, ref in mine.items()}}
    mine_two = {3: far2.at[0], 4: x2.at[0], 5: x2.at[1], 8: far2.at[1]}
    two = {6: near2.at[0], 7: near2.at[1], **{n: (ref, ref) for n, ref in mine_two.items()}}

    def flag_of(n):
        return low if n < 4 else high if n > 7 else None

    def vector(i):
        for n, count in ((2, half), (3, None), (4, None), (9, half)):
            value = step_of(
                scale_ref[...], diag_ref[n - 2], *[pick(fields[m], part, i) for m in (n - 1, n, n + 1)],
                None, 0.0, flag_of(n), count)
            mine[n][i, pl.ds(0, value.shape[0])] = value
        for n, count in ((3, half), (4, None), (5, None), (8, half)):
            value = step_of(
                scale_ref[...], diag_ref[n - 2], *[pick(one[m], part, i) for m in (n - 1, n, n + 1)],
                pick(fields[n], part, i), BETA[1], flag_of(n), count)
            mine_two[n][i, pl.ds(0, value.shape[0])] = value
        for n in (4, 5, 6, 7):
            x3[n - 4, i] = step_of(
                scale_ref[...], diag_ref[n - 2], *[pick(two[m], part, i) for m in (n - 1, n, n + 1)],
                pick(one[n], part, i), BETA[2], None, half)

    half_loop(vector)
    if part == 0:
        return
    copies = []
    for n, (x1_half, x2_half) in enumerate(((x1_first, x2_first), (x1, x2))):
        vectors = pl.ds(n * (BLK // 2), BLK // 2)
        copies.append(pltpu.make_async_copy(x1_half.at[:, pl.ds(0, half)], x1_out.at[vectors], sems.at[2 * n]))
        copies.append(pltpu.make_async_copy(
            x2_half.at[:, :, pl.ds(0, half)], x2_out.at[:, vectors], sems.at[2 * n + 1]))
    for copy in copies:
        copy.start()
    views = (fields, {**one, 4: (x1_first, x1)},
             {**two, 4: (x2_first.at[0], x2.at[0]), 5: (x2_first.at[1], x2.at[1])},
             {n: (x3_first.at[n - 4], x3.at[n - 4]) for n in (4, 5, 6, 7)})
    upper = blocks * (blocks + 1) // 2
    acc[pl.ds(0, upper)] = start[pl.ds(0, upper)]
    for moment, layers in LATE.items():
        gram_part(acc, views, moment, layers, blocks, half, width, start if moment in EARLY else None)
    total = jnp.sum(acc[...], axis=1)
    sums = lax.dot_general(
        jnp.ones((8, 128), jnp.float32), total, (((1,), (1,)), ((), ())),
        precision=HIGHEST, preferred_element_type=jnp.float32)
    nu_out[...] = jnp.broadcast_to(sums[:1][None], nu_out.shape)
    for copy in copies:
        copy.wait()


def with_affine(kernel, *refs, **static):
    kernel(*refs[1:], affine=refs[0], **static)


def kernels(blocks, half, width, peers, affine):
    rows = half + 2 * EDGE
    moments = 2 * ITERS + 1
    count = blocks * (blocks + 1) // 2
    vmem = pl.BlockSpec(memory_space=pltpu.VMEM)
    hbm = pl.BlockSpec(memory_space=pltpu.HBM)
    sizes = dict(blocks=blocks, half=half, width=width)
    layer = (blocks, rows, width)
    part_layer = (blocks // 2, rows, width)
    cells = blocks * rows * width

    def out(*shape):
        return jax.ShapeDtypeStruct(shape, jnp.float32)

    def far(*shape):
        return pltpu.HBM(shape, jnp.float32)

    def scales(number):
        return [pltpu.VMEM((rows, width), jnp.float32), pltpu.VMEM((number, rows, width), jnp.float32)]

    def call(kernel, arrays, outs, scratch, mib, ops, **static):
        if affine is None:
            run, lead = functools.partial(kernel, affine=None, **sizes, **static), ()
        else:
            run, lead = functools.partial(with_affine, kernel, **sizes, **static), (affine,)
        return pl.pallas_call(
            run,
            out_shape=outs,
            in_specs=[pl.BlockSpec(memory_space=pltpu.SMEM)] * len(lead) + [vmem] * len(arrays),
            out_specs=tuple(vmem if isinstance(o, jax.ShapeDtypeStruct) else hbm for o in outs),
            scratch_shapes=scratch,
            compiler_params=pltpu.CompilerParams(vmem_limit_bytes=mib << 20),
            cost_estimate=pl.CostEstimate(flops=ops * cells, bytes_accessed=16 * cells, transcendentals=0),
        )(*lead, *arrays)

    def zero(arrays, layers, add):
        return call(zero_kernel, arrays, (out(count, 8, 128),), [], 4, 20, layers=layers, add=add)[0]

    def first(arrays, part):
        return call(first_kernel, arrays, (out(2, *part_layer), far(2, blocks // 2, half, width)),
                    scales(2) + [pltpu.SemaphoreType.DMA], 8, 20, part=part)

    def early(*arrays):
        outs = (out(2, *layer), out(2, *layer), far(blocks, half, width), far(blocks, half, width),
                out(len(EARLY) * count, 8, 128), far(blocks, half, width))
        return call(early_kernel, arrays, outs, scales(4) + [pltpu.SemaphoreType.DMA((3,))], 12, 200)

    def late(arrays, part):
        mine = ((part_layer), (2, *part_layer), (4, blocks // 2, half, width))
        work = [pltpu.VMEM((3, *part_layer), jnp.float32), pltpu.VMEM((2, *part_layer), jnp.float32)]
        if part == 0:
            return call(late_kernel, arrays, tuple(out(*m) for m in mine), work + scales(8), 12, 100, part=0)
        outs = (far(blocks, half, width), far(2, blocks, half, width), out(peers, 1, moments * count))
        work = [pltpu.VMEM(m, jnp.float32) for m in mine] + work + [
            pltpu.VMEM((moments * count, 8, 128), jnp.float32), *scales(8), pltpu.SemaphoreType.DMA((4,))]
        return call(late_kernel, arrays, outs, work, 18, 200, part=1)

    return zero, first, early, late


def moment_tables(blocks):
    b1, b2 = BETA[1], BETA[2]
    size = 2 * ITERS + 1
    unit = np.eye(size)
    g02 = unit[2] - b1 * unit[0]
    g03 = unit[3] - b2 * unit[1]
    g13 = unit[4] + b1 * g02 - b2 * unit[2]
    table = [[unit[0], unit[1], g02, g03], [unit[1], unit[2], unit[3], g13],
             [g02, unit[3], unit[4], unit[5]], [g03, g13, unit[5], unit[6]]]
    pairs_of = [(m, v, w) for m in range(size) for v in range(blocks) for w in range(v, blocks)]
    rows = np.zeros((3, blocks, len(pairs_of)), np.float32)
    cols = np.zeros((2, len(pairs_of), ITERS + 1, ITERS + 1, blocks), np.float32)
    for n, (m, v, w) in enumerate(pairs_of):
        rows[0, v, n] = 1.0
        rows[1, w, n] = float(v != w)
        if v == w and m < 3:
            rows[2, m, n] = 1.0
        for i in range(ITERS + 1):
            for j in range(ITERS + 1):
                cols[0, n, i, j, w] = table[i][j][m]
                cols[1, n, i, j, v] = table[i][j][m]
    return rows, cols.reshape(2, len(pairs_of), -1)


def shift_tables(blocks):
    table = np.zeros((2, ITERS, ITERS + 1))
    for k in range(ITERS):
        table[0, k, k + 1] = 1.0
        table[1, k, k] = 1.0
        if k:
            table[0, k, k - 1] = BETA[k]
    return np.stack([np.kron(t, np.eye(blocks)) for t in table]).astype(np.float32)


def contract(left, right, at_left, at_right):
    return lax.dot_general(left, right, (((at_left,), (at_right,)), ((), ())),
                           precision=HIGHEST, preferred_element_type=jnp.float32)


def solve_small(parts, rows, cols, shift, blocks):
    nu = jnp.sum(parts, axis=0)
    traces = jnp.sum(rows[2] * nu, axis=1, keepdims=True)
    mean = traces[1:2] / traces[:1]
    spread = jnp.sqrt(jnp.maximum(traces[2:3] / traces[:1] - mean * mean, 1e-6))
    again = jnp.logical_or(spread < 0.35, jnp.abs(mean) > 3.0 * spread)
    fit = (jnp.max(jnp.where(again, 1, 0)), jnp.max(mean), jnp.max(spread))
    wide = sum(contract(rows[n] * nu, cols[n].astype(jnp.float32), 1, 0) for n in range(2))
    total, size = (ITERS + 1) * blocks, ITERS * blocks
    gram = jnp.concatenate([wide[:, total * i:total * i + total] for i in range(ITERS + 1)], axis=0)
    row = lax.broadcasted_iota(jnp.int32, (total, total), 0)
    col = lax.broadcasted_iota(jnp.int32, (total, total), 1)
    eye = jnp.where(row == col, 1.0, 0.0)
    moved = contract(shift, gram, 1, 0)
    factors = jnp.concatenate([gram, eye], axis=1)
    solving = jnp.concatenate([contract(moved, shift, 1, 1), moved[:, :blocks]], axis=1)
    below = lax.broadcasted_iota(jnp.int32, factors.shape, 0)
    here = lax.broadcasted_iota(jnp.int32, solving.shape, 0)
    for j in range(total - 1):
        scale = factors[j:j + 1] / factors[j:j + 1, j:j + 1]
        factors = factors - jnp.where(below > j, factors[:, j:j + 1], 0.0) * scale
        if j < size:
            pivot = solving[j:j + 1] / solving[j:j + 1, j:j + 1]
            solving = jnp.where(here == j, pivot, solving - solving[:, j:j + 1] * pivot)
    pivots = jnp.sum(factors[:, :total] * eye, axis=1, keepdims=True)
    factors = factors / jnp.sqrt(pivots)
    upper = jnp.where(row <= col, factors[:, :total], 0.0)
    inverse = factors[:size, total:total + size]
    hessenberg = contract(inverse, contract(shift, upper, 1, 1), 1, 0)
    row = lax.broadcasted_iota(jnp.int32, hessenberg.shape, 0) // blocks
    col = lax.broadcasted_iota(jnp.int32, hessenberg.shape, 1) // blocks
    return jnp.where(col <= row + 1, hessenberg, 0.0), solving[:, size:], fit


def blend(buffer, terms, splat, blocks, half, width):
    def tile(step, carry):
        at = pl.multiple_of(step * 8, 8)
        parts = [pl.ds(128 * c, 128) for c in range(width // 128)]
        sums = [[None] * len(parts) for _ in range(blocks)]
        for k, term in enumerate(terms):
            for v in range(blocks):
                values = [term[v, pl.ds(at, 8), lanes] for lanes in parts]
                for w in range(blocks):
                    scale = jnp.broadcast_to(splat[w, pl.ds(k * blocks + v, 1), :], (8, 128))
                    for c, value in enumerate(values):
                        value = scale * value
                        sums[w][c] = value if sums[w][c] is None else sums[w][c] + value
        for w in range(blocks):
            for c, lanes in enumerate(parts):
                buffer[w, pl.ds(at, 8), lanes] = sums[w][c]
        return carry

    lax.fori_loop(0, half // 8, tile, 0)


def place_of(n, half):
    parity = lax.rem(lax.axis_index("gz"), 2)
    layer = (parity, 1 - parity, 1 - parity, parity)[n]
    rows = (parity, parity, 1 - parity, 1 - parity)[n]
    return layer, pl.ds(pl.multiple_of(rows * half, 8), half)


TERMS = (((0, None), (1, None), (2, 0)), ((3, None), (4, None), (2, 1)))


def finish_kernel(parts, rows, cols, shift, *refs, blocks, half, width):
    arrays, (hess_out, splat, out, again_out, affine_out, source, buffer, sems, out_sems) = refs[:5], refs[5:]
    copies = []
    for n, terms in enumerate(TERMS):
        for k, (ref, at) in enumerate(terms):
            ref = arrays[ref] if at is None else arrays[ref].at[at]
            copy = pltpu.make_async_copy(
                ref.at[pl.ds(0, blocks), pl.ds(0, half)], source.at[n, k], sems.at[n, k])
            copy.start()
            copies.append(copy)
    hessenberg, weights, (again, mean, spread) = solve_small(parts[...], rows, cols, shift[...], blocks)
    again_out[0, 0] = again
    affine_out[0, 0] = mean
    affine_out[0, 1] = spread
    hess_out[...] = hessenberg
    for w in range(blocks):
        splat[w] = jnp.broadcast_to(weights[:, w:w + 1], (ITERS * blocks, 128))
    for copy in copies:
        copy.wait()
    sends = []
    for n in range(len(TERMS)):
        blend(buffer.at[n], [source.at[n, k] for k in range(ITERS)], splat, blocks, half, width)
        layer, at = place_of(n, half)
        sends.append(pltpu.make_async_copy(buffer.at[n], out.at[:, layer, at], out_sems.at[n]))
        sends[-1].start()
    for send in sends:
        send.wait()


def others_kernel(splat, near0, far0, one_first, one_second, near2, far2, _, out, source, buffer, sems, out_sems, *,
                  blocks, half, width):
    loads = []
    for n, (zero, two) in enumerate(((near0, near2), (far0, far2))):
        for k, (term, at) in enumerate((
            (zero.at[pl.ds(0, blocks), pl.ds(0, half)], source.at[n, 0]),
            (one_first.at[n], source.at[n, 1, pl.ds(0, blocks // 2)]),
            (one_second.at[n], source.at[n, 1, pl.ds(blocks // 2, blocks // 2)]),
            (two, source.at[n, 2]),
        )):
            loads.append(pltpu.make_async_copy(term, at, sems.at[n, k]))
            loads[-1].start()
    sends = []
    for n in range(2):
        for load in loads[4 * n:4 * n + 4]:
            load.wait()
        blend(buffer.at[n], [source.at[n, k] for k in range(ITERS)], splat, blocks, half, width)
        layer, at = place_of(2 + n, half)
        sends.append(pltpu.make_async_copy(buffer.at[n], out.at[:, layer, at], out_sems.at[n]))
        sends[-1].start()
    for send in sends:
        send.wait()


def in_hbm(array):
    return pltpu.with_memory_space_constraint(array, pltpu.HBM)


def finish(parts, arrays, blocks, half, width, affine):
    vmem = pl.BlockSpec(memory_space=pltpu.VMEM)
    hbm = pl.BlockSpec(memory_space=pltpu.HBM)
    smem = pl.BlockSpec(memory_space=pltpu.SMEM)
    rows, cols = moment_tables(blocks)
    tables = shift_tables(blocks)
    if affine is None:
        shift = (SPREAD * tables[0] + CENTER * tables[1]).astype(np.float32)
    else:
        shift = tables[0] / affine[0, 1] + tables[1] * affine[0, 0]
    size = ITERS * blocks
    piece = (blocks, half, width)
    return pl.pallas_call(
        functools.partial(finish_kernel, blocks=blocks, half=half, width=width),
        out_shape=(
            jax.ShapeDtypeStruct((size, size + blocks), jnp.float32),
            jax.ShapeDtypeStruct((blocks, size, 128), jnp.float32),
            jax.ShapeDtypeStruct((blocks, 2, 2 * half, width), jnp.float32),
            jax.ShapeDtypeStruct((1, 1), jnp.int32),
            jax.ShapeDtypeStruct((1, 2), jnp.float32),
        ),
        in_specs=[vmem] * 4 + [hbm] * len(arrays),
        out_specs=(vmem, vmem, hbm, smem, smem),
        scratch_shapes=[
            pltpu.VMEM((len(TERMS), ITERS, *piece), jnp.float32),
            pltpu.VMEM((len(TERMS), *piece), jnp.float32),
            pltpu.SemaphoreType.DMA((len(TERMS), ITERS)),
            pltpu.SemaphoreType.DMA((len(TERMS),)),
        ],
        compiler_params=pltpu.CompilerParams(vmem_limit_bytes=16 << 20),
        cost_estimate=pl.CostEstimate(flops=300 * blocks * half * width, bytes_accessed=1 << 23, transcendentals=0),
        name="finish",
    )(parts, rows, cols.astype(jnp.bfloat16), shift, *[in_hbm(array) for array in arrays])


def others(splat, near0, far0, one_first, one_second, near2, far2, result, half, width):
    vmem = pl.BlockSpec(memory_space=pltpu.VMEM)
    hbm = pl.BlockSpec(memory_space=pltpu.HBM)
    blocks = near2.shape[0]
    return pl.pallas_call(
        functools.partial(others_kernel, blocks=blocks, half=half, width=width),
        out_shape=jax.ShapeDtypeStruct(result.shape, result.dtype),
        in_specs=[vmem] + [hbm] * 2 + [pl.BlockSpec(memory_space=pl.ANY)] * 4 + [hbm],
        out_specs=hbm,
        scratch_shapes=[
            pltpu.VMEM((2, ITERS, blocks, half, width), jnp.float32),
            pltpu.VMEM((2, blocks, half, width), jnp.float32),
            pltpu.SemaphoreType.DMA((2, 4)),
            pltpu.SemaphoreType.DMA((2,)),
        ],
        input_output_aliases={7: 0},
        compiler_params=pltpu.CompilerParams(vmem_limit_bytes=8 << 20),
        name="others",
    )(splat, in_hbm(near0), in_hbm(far0), one_first, one_second, near2, far2, result)


def attempt(right_side, diagonal, affine=None):
    blocks, _, ny, width = right_side.shape
    half = ny // 2
    peers_z, peers_y = lax.axis_size("gz"), lax.axis_size("gy")
    even = lax.axis_index("gz") % 2 == 0
    field = jnp.concatenate([right_side, diagonal[None]], axis=0)
    above = lax.ppermute(field[:, :, ny - EDGE:], "gy", pairs(peers_y, 1))
    under = lax.ppermute(field[:, :, :EDGE], "gy", pairs(peers_y, -1))
    first = jnp.concatenate([field[:, :, :half + EDGE], above], axis=2)
    second = jnp.concatenate([field[:, :, half:], under, field[:, :, half - EDGE:half]], axis=2)

    swap = swap_pairs(peers_z, 1)
    inward = [(i, j) for i, j in pairs(peers_z, 2) if i % 2 == 0] + [(i, j) for i, j in pairs(peers_z, -2) if i % 2]
    outward = [(j, i) for i, j in inward]
    send_near = jnp.where(even, second[:, 1], first[:, 0])
    send_far = jnp.where(even, second[:, 0], first[:, 1])
    keep_near = jnp.where(even, first[:, 1], second[:, 0])
    keep_far = jnp.where(even, first[:, 0], second[:, 1])
    zero, first_step, early, late = kernels(blocks, half, width, peers_z * peers_y, affine)

    def move(array, links):
        return lax.ppermute(array, "gz", links)

    middle = blocks // 2
    got_near = move(send_near, swap)
    in_one = move(keep_near[:blocks, :half], inward)
    out_one = move(keep_far, outward)
    far_a = move(jnp.concatenate([send_far[:middle], send_far[blocks:]], axis=0), swap)
    far_b = move(send_far[middle:blocks], swap)
    out_two = move(keep_near, outward)
    in_two = move(got_near, inward)
    out_a = move(got_near[:middle, :half], outward)
    out_b = move(got_near[middle:blocks, :half], outward)
    nu_zero = zero((keep_far, keep_near), (4, 5), False)
    mid_a, sent_a = first_step((keep_near, got_near, far_a, far_a, out_one), 0)
    back_a = move(sent_a, swap)
    in_a = move(far_a, inward)
    nu_zero = zero((got_near, nu_zero), (6,), True)
    mid_b, sent_b = first_step((keep_near, got_near, far_a, far_b, out_one), 1)
    back_b = move(sent_b, swap)
    in_b = move(far_b, inward)
    near1, near2, near_sent, far_sent, start, x1_near = early(
        keep_far, keep_near, got_near, far_a, far_b, out_one, out_two, mid_a, mid_b, nu_zero)
    near_back2 = move(near_sent, swap)
    first_half = late((in_one, in_two, in_a, keep_far, keep_near, got_near, far_a, far_b, out_one, out_two,
                       out_a, mid_a, mid_b, near1, near2), 0)
    x1_far, x2, nu = late((in_one, in_two, in_b, keep_far, keep_near, got_near, far_a, far_b, out_one, out_two,
                           out_b, mid_a, mid_b, near1, near2, in_a, *first_half, start), 1)
    parts = lax.all_to_all(nu, ("gz", "gy"), 0, 0)
    far_back2 = move(far_sent, swap)
    hessenberg, splat, result, again, fit = finish(
        parts, (keep_far, x1_far, x2, keep_near, x1_near), blocks, half, width, affine)
    result = others(splat, send_near, send_far, back_a, back_b, near_back2, far_back2, result, half, width)
    return result, hessenberg, again, fit


def body(right_side, diagonal):
    result, hessenberg, again, fit = attempt(right_side, diagonal)

    def repeat(right_side, diagonal, fit, result, hessenberg):
        affine = jnp.stack([CENTER + SPREAD * fit[0, 0], 1.0 / (SPREAD * fit[0, 1])]).reshape(1, 2)
        return attempt(right_side, diagonal, affine)[:2]

    def accept(right_side, diagonal, fit, result, hessenberg):
        return result, hessenberg

    return lax.cond(again[0, 0] != 0, repeat, accept, right_side, diagonal, fit, result, hessenberg)


def solution(mesh):
    in_specs = (P(None, "gz", "gy", None), P("gz", "gy", None))
    out_specs = (P(None, "gz", "gy", None), P())

    return jax.shard_map(body, mesh=mesh, in_specs=in_specs, out_specs=out_specs, check_vma=False)
```

```python
import functools

import jax
import jax.numpy as jnp
import numpy as np
from jax import lax
from jax.experimental import pallas as pl
from jax.experimental.pallas import tpu as pltpu
from jax.sharding import PartitionSpec as P

BLK = 8
ITERS = 3
EDGE = 4
CENTER, SPREAD = 7.6, 2.6
BETA = (0.0, 1.0, 1.5)
HIGHEST = lax.Precision.HIGHEST


def pairs(peers, step):
    return [(i, i + step) for i in range(peers) if 0 <= i + step < peers]


def swap_pairs(peers, bit):
    return [(i, i ^ bit) for i in range(peers)]


def row_masks(half, width):
    rows = half + 2 * EDGE
    parity = lax.rem(lax.axis_index("gz"), 2)
    at_y = lax.axis_index("gy")
    no_below = jnp.logical_and(at_y == lax.axis_size("gy") - 1, parity == 1)
    no_above = jnp.logical_and(at_y == 0, parity == 0)
    row = lax.broadcasted_iota(jnp.int32, (rows, width), 0)
    below = jnp.where(no_below, 0.0, 1.0)
    above = jnp.where(no_above, 0.0, 1.0)
    return jnp.where(row < half, 1.0, jnp.where(row < half + EDGE, below, above))


def side_flags():
    place = lax.axis_index("gz")
    parity = lax.rem(place, 2)
    downward = jnp.where(place >= 2, 1.0, 0.0)
    upward = jnp.where(place < lax.axis_size("gz") - 2, 1.0, 0.0)
    return (jnp.where(parity == 0, downward, upward), jnp.where(parity == 0, upward, downward))


def pick(view, part, i):
    return view[part][i] if isinstance(view, tuple) else view[i + part * (BLK // 2)]


def entry(view, v, rows, lanes):
    half = BLK // 2
    return view[v // half][v % half, rows, lanes] if isinstance(view, tuple) else view[v, rows, lanes]


def diag_of(view):
    return view[0][BLK // 2] if isinstance(view, tuple) else view[BLK]


def set_scales(scale_ref, diag_ref, fields, slots, half, width, affine):
    center, inverse = (CENTER, 1.0 / SPREAD) if affine is None else (affine[0, 0], affine[0, 1])
    scale_ref[...] = row_masks(half, width) * inverse
    low, high = side_flags()
    for slot, layer in enumerate(slots):
        value = scale_ref[...] * (diag_of(fields[layer]) + (6.0 - center))
        if layer < 4:
            value = value * low
        if layer > 7:
            value = value * high
        diag_ref[slot] = value


def step_of(scale, diag, low, mid, high, before, beta, flag=None, count=None):
    rows, width = mid.shape
    count = count or rows
    own = mid[:count]
    lane = lax.broadcasted_iota(jnp.int32, (count, width), 1)
    beside = low[:count] + high[:count]
    beside = beside + pltpu.roll(mid, 1, 0)[:count] + pltpu.roll(mid, rows - 1, 0)[:count]
    beside = beside + jnp.where(lane == 0, 0.0, pltpu.roll(own, 1, 1))
    beside = beside + jnp.where(lane == width - 1, 0.0, pltpu.roll(own, width - 1, 1))
    scale = scale[:count]
    if flag is not None:
        scale = scale * flag
    value = diag[:count] * own - scale * beside
    if beta:
        value = value - beta * before[:count]
    return value


def gram_part(acc, views, moment, layers, blocks, half, width, start):
    left, right = views[moment // 2], views[(moment + 1) // 2]
    upper = [(v, w) for v in range(blocks) for w in range(v, blocks)]

    def spot(step, sums):
        at = pl.ds(pl.multiple_of(step * 8, 8), 8)
        sums = list(sums)
        for layer in layers:
            for c in range(width // 128):
                lanes = pl.ds(128 * c, 128)
                rights = [entry(right[layer], w, at, lanes) for w in range(blocks)]
                for v in range(blocks):
                    one = rights[v] if left is right else entry(left[layer], v, at, lanes)
                    for n, (a, b) in enumerate(upper):
                        if a == v:
                            sums[n] = sums[n] + one * rights[b]
        return tuple(sums)

    zeros = tuple(jnp.zeros((8, 128), jnp.float32) for _ in upper)
    sums = lax.fori_loop(0, half // 8, spot, zeros)
    base = moment * len(upper)
    for n in range(len(upper)):
        acc[base + n] = sums[n] if start is None else sums[n] + start[base + n]


def half_loop(body):
    lax.fori_loop(0, BLK // 2, lambda i, carry: (body(i), carry)[1], 0)


EARLY = {0: (7,), 1: (5, 6, 7), 2: (5, 6, 7), 3: (6, 7), 4: (6, 7)}
LATE = {1: (4,), 2: (4,), 3: (4, 5), 4: (4, 5), 5: (4, 5, 6, 7), 6: (4, 5, 6, 7)}


def first_kernel(*refs, affine, part, blocks, half, width):
    near, mid, far_one, far_two, out_one, x1, sent, scale_ref, diag_ref, sem = refs
    fields = {5: near, 6: mid, 7: (far_one, far_two), 8: out_one}
    set_scales(scale_ref, diag_ref, fields, (6, 7), half, width, affine)

    def vector(i):
        for slot, n in enumerate((6, 7)):
            x1[slot, i] = step_of(
                scale_ref[...], diag_ref[slot], *[pick(fields[m], part, i) for m in (n - 1, n, n + 1)], None, 0.0)

    half_loop(vector)
    copy = pltpu.make_async_copy(x1.at[:, :, pl.ds(0, half)], sent, sem)
    copy.start()
    copy.wait()


def zero_kernel(*refs, affine, layers, add, blocks, half, width):
    fields = dict(zip(layers, refs))
    gram_part(refs[-1], (fields,), 0, layers, blocks, half, width, refs[len(layers)] if add else None)


def early_kernel(*refs, affine, blocks, half, width):
    (keep_far, keep_near, got_near, far_one, far_two, out_one, out_two, mid_one, mid_two, start,
     x1, x2, near_sent, far_sent, acc, x1_out, scale_ref, diag_ref, sems) = refs
    fields = {4: keep_far, 5: keep_near, 6: got_near, 7: (far_one, far_two), 8: out_one, 9: out_two}
    slots = (5, 6, 7, 8)
    set_scales(scale_ref, diag_ref, fields, slots, half, width, affine)
    flag = side_flags()[1]
    one = {5: x1.at[0], 6: (mid_one.at[0], mid_two.at[0]), 7: (mid_one.at[1], mid_two.at[1]), 8: x1.at[1]}

    def vector(i):
        for part in range(2):
            v = i + part * (BLK // 2)
            for n in (5, 8):
                one[n][v] = step_of(
                    scale_ref[...], diag_ref[n - 5], *[pick(fields[m], part, i) for m in (n - 1, n, n + 1)],
                    None, 0.0, flag if n == 8 else None)
            for slot, n in enumerate((6, 7)):
                x2[slot, v] = step_of(
                    scale_ref[...], diag_ref[n - 5], *[pick(one[m], part, i) for m in (n - 1, n, n + 1)],
                    pick(fields[n], part, i), BETA[1])

    half_loop(vector)
    copies = [pltpu.make_async_copy(ref.at[:, pl.ds(0, half)], out, sems.at[n]) for n, (ref, out) in enumerate(
        ((x2.at[0], near_sent), (x2.at[1], far_sent), (x1.at[0], x1_out)))]
    for copy in copies:
        copy.start()
    views = (fields, one, {n: x2.at[n - 6] for n in (6, 7)})
    for moment, layers in EARLY.items():
        gram_part(acc, views, moment, layers, blocks, half, width, start if moment == 0 else None)
    for copy in copies:
        copy.wait()


def late_kernel(*refs, affine, part, blocks, half, width):
    (in_one, in_two, in_three, keep_far, keep_near, got_near, far_one, far_two, out_one, out_two, out_three,
     mid_one, mid_two, near1, near2) = refs[:15]
    rest = refs[15:]
    if part == 0:
        x1, x2, x3, far1, far2, scale_ref, diag_ref = rest
        third = (in_three,)
    else:
        (before, x1_first, x2_first, x3_first, start, x1_out, x2_out, nu_out,
         x1, x2, x3, far1, far2, acc, scale_ref, diag_ref, sems) = rest
        third = (before, in_three)
    third = third + (None,) * (2 - len(third))
    fields = {1: in_one, 2: in_two, 3: third, 4: keep_far, 5: keep_near, 6: got_near, 7: (far_one, far_two),
              8: out_one, 9: out_two, 10: (out_three, out_three)}
    slots = tuple(range(2, 10))
    set_scales(scale_ref, diag_ref, fields, slots, half, width, affine)
    low, high = side_flags()
    mine = {2: far1.at[0], 3: far1.at[1], 4: x1, 9: far1.at[2]}
    one = {5: near1.at[0], 8: near1.at[1], 6: (mid_one.at[0], mid_two.at[0]), 7: (mid_one.at[1], mid_two.at[1]),
           **{n: (ref, ref) for n, ref in mine.items()}}
    mine_two = {3: far2.at[0], 4: x2.at[0], 5: x2.at[1], 8: far2.at[1]}
    two = {6: near2.at[0], 7: near2.at[1], **{n: (ref, ref) for n, ref in mine_two.items()}}

    def flag_of(n):
        return low if n < 4 else high if n > 7 else None

    def vector(i):
        for n, count in ((2, half), (3, None), (4, None), (9, half)):
            value = step_of(
                scale_ref[...], diag_ref[n - 2], *[pick(fields[m], part, i) for m in (n - 1, n, n + 1)],
                None, 0.0, flag_of(n), count)
            mine[n][i, pl.ds(0, value.shape[0])] = value
        for n, count in ((3, half), (4, None), (5, None), (8, half)):
            value = step_of(
                scale_ref[...], diag_ref[n - 2], *[pick(one[m], part, i) for m in (n - 1, n, n + 1)],
                pick(fields[n], part, i), BETA[1], flag_of(n), count)
            mine_two[n][i, pl.ds(0, value.shape[0])] = value
        for n in (4, 5, 6, 7):
            x3[n - 4, i] = step_of(
                scale_ref[...], diag_ref[n - 2], *[pick(two[m], part, i) for m in (n - 1, n, n + 1)],
                pick(one[n], part, i), BETA[2], None, half)

    half_loop(vector)
    if part == 0:
        return
    copies = []
    for n, (x1_half, x2_half) in enumerate(((x1_first, x2_first), (x1, x2))):
        vectors = pl.ds(n * (BLK // 2), BLK // 2)
        copies.append(pltpu.make_async_copy(x1_half.at[:, pl.ds(0, half)], x1_out.at[vectors], sems.at[2 * n]))
        copies.append(pltpu.make_async_copy(
            x2_half.at[:, :, pl.ds(0, half)], x2_out.at[:, vectors], sems.at[2 * n + 1]))
    for copy in copies:
        copy.start()
    views = (fields, {**one, 4: (x1_first, x1)},
             {**two, 4: (x2_first.at[0], x2.at[0]), 5: (x2_first.at[1], x2.at[1])},
             {n: (x3_first.at[n - 4], x3.at[n - 4]) for n in (4, 5, 6, 7)})
    upper = blocks * (blocks + 1) // 2
    acc[pl.ds(0, upper)] = start[pl.ds(0, upper)]
    for moment, layers in LATE.items():
        gram_part(acc, views, moment, layers, blocks, half, width, start if moment in EARLY else None)
    total = jnp.sum(acc[...], axis=1)
    sums = lax.dot_general(
        jnp.ones((8, 128), jnp.float32), total, (((1,), (1,)), ((), ())),
        precision=HIGHEST, preferred_element_type=jnp.float32)
    nu_out[...] = jnp.broadcast_to(sums[:1][None], nu_out.shape)
    for copy in copies:
        copy.wait()


def with_affine(kernel, *refs, **static):
    kernel(*refs[1:], affine=refs[0], **static)


def kernels(blocks, half, width, peers, affine):
    rows = half + 2 * EDGE
    moments = 2 * ITERS + 1
    count = blocks * (blocks + 1) // 2
    vmem = pl.BlockSpec(memory_space=pltpu.VMEM)
    hbm = pl.BlockSpec(memory_space=pltpu.HBM)
    sizes = dict(blocks=blocks, half=half, width=width)
    layer = (blocks, rows, width)
    part_layer = (blocks // 2, rows, width)
    cells = blocks * rows * width

    def out(*shape):
        return jax.ShapeDtypeStruct(shape, jnp.float32)

    def far(*shape):
        return pltpu.HBM(shape, jnp.float32)

    def scales(number):
        return [pltpu.VMEM((rows, width), jnp.float32), pltpu.VMEM((number, rows, width), jnp.float32)]

    def call(kernel, arrays, outs, scratch, mib, ops, **static):
        if affine is None:
            run, lead = functools.partial(kernel, affine=None, **sizes, **static), ()
        else:
            run, lead = functools.partial(with_affine, kernel, **sizes, **static), (affine,)
        return pl.pallas_call(
            run,
            out_shape=outs,
            in_specs=[pl.BlockSpec(memory_space=pltpu.SMEM)] * len(lead) + [vmem] * len(arrays),
            out_specs=tuple(vmem if isinstance(o, jax.ShapeDtypeStruct) else hbm for o in outs),
            scratch_shapes=scratch,
            compiler_params=pltpu.CompilerParams(vmem_limit_bytes=mib << 20),
            cost_estimate=pl.CostEstimate(flops=ops * cells, bytes_accessed=16 * cells, transcendentals=0),
        )(*lead, *arrays)

    def zero(arrays, layers, add):
        return call(zero_kernel, arrays, (out(count, 8, 128),), [], 4, 20, layers=layers, add=add)[0]

    def first(arrays, part):
        return call(first_kernel, arrays, (out(2, *part_layer), far(2, blocks // 2, half, width)),
                    scales(2) + [pltpu.SemaphoreType.DMA], 8, 20, part=part)

    def early(*arrays):
        outs = (out(2, *layer), out(2, *layer), far(blocks, half, width), far(blocks, half, width),
                out(len(EARLY) * count, 8, 128), far(blocks, half, width))
        return call(early_kernel, arrays, outs, scales(4) + [pltpu.SemaphoreType.DMA((3,))], 12, 200)

    def late(arrays, part):
        mine = ((part_layer), (2, *part_layer), (4, blocks // 2, half, width))
        work = [pltpu.VMEM((3, *part_layer), jnp.float32), pltpu.VMEM((2, *part_layer), jnp.float32)]
        if part == 0:
            return call(late_kernel, arrays, tuple(out(*m) for m in mine), work + scales(8), 12, 100, part=0)
        outs = (far(blocks, half, width), far(2, blocks, half, width), out(peers, 1, moments * count))
        work = [pltpu.VMEM(m, jnp.float32) for m in mine] + work + [
            pltpu.VMEM((moments * count, 8, 128), jnp.float32), *scales(8), pltpu.SemaphoreType.DMA((4,))]
        return call(late_kernel, arrays, outs, work, 18, 200, part=1)

    return zero, first, early, late


def moment_tables(blocks):
    b1, b2 = BETA[1], BETA[2]
    size = 2 * ITERS + 1
    unit = np.eye(size)
    g02 = unit[2] - b1 * unit[0]
    g03 = unit[3] - b2 * unit[1]
    g13 = unit[4] + b1 * g02 - b2 * unit[2]
    table = [[unit[0], unit[1], g02, g03], [unit[1], unit[2], unit[3], g13],
             [g02, unit[3], unit[4], unit[5]], [g03, g13, unit[5], unit[6]]]
    pairs_of = [(m, v, w) for m in range(size) for v in range(blocks) for w in range(v, blocks)]
    rows = np.zeros((3, blocks, len(pairs_of)), np.float32)
    cols = np.zeros((2, len(pairs_of), ITERS + 1, ITERS + 1, blocks), np.float32)
    for n, (m, v, w) in enumerate(pairs_of):
        rows[0, v, n] = 1.0
        rows[1, w, n] = float(v != w)
        if v == w and m < 3:
            rows[2, m, n] = 1.0
        for i in range(ITERS + 1):
            for j in range(ITERS + 1):
                cols[0, n, i, j, w] = table[i][j][m]
                cols[1, n, i, j, v] = table[i][j][m]
    return rows, cols.reshape(2, len(pairs_of), -1)


def shift_tables(blocks):
    table = np.zeros((2, ITERS, ITERS + 1))
    for k in range(ITERS):
        table[0, k, k + 1] = 1.0
        table[1, k, k] = 1.0
        if k:
            table[0, k, k - 1] = BETA[k]
    return np.stack([np.kron(t, np.eye(blocks)) for t in table]).astype(np.float32)


def contract(left, right, at_left, at_right):
    return lax.dot_general(left, right, (((at_left,), (at_right,)), ((), ())),
                           precision=HIGHEST, preferred_element_type=jnp.float32)


def solve_small(parts, rows, cols, shift, blocks):
    nu = jnp.sum(parts, axis=0)
    traces = jnp.sum(rows[2] * nu, axis=1, keepdims=True)
    mean = traces[1:2] / traces[:1]
    spread = jnp.sqrt(jnp.maximum(traces[2:3] / traces[:1] - mean * mean, 1e-6))
    again = jnp.logical_or(spread < 0.35, jnp.abs(mean) > 3.0 * spread)
    fit = (jnp.max(jnp.where(again, 1, 0)), jnp.max(mean), jnp.max(spread))
    wide = sum(contract(rows[n] * nu, cols[n].astype(jnp.float32), 1, 0) for n in range(2))
    total, size = (ITERS + 1) * blocks, ITERS * blocks
    gram = jnp.concatenate([wide[:, total * i:total * i + total] for i in range(ITERS + 1)], axis=0)
    row = lax.broadcasted_iota(jnp.int32, (total, total), 0)
    col = lax.broadcasted_iota(jnp.int32, (total, total), 1)
    eye = jnp.where(row == col, 1.0, 0.0)
    moved = contract(shift, gram, 1, 0)
    factors = jnp.concatenate([gram, eye], axis=1)
    solving = jnp.concatenate([contract(moved, shift, 1, 1), moved[:, :blocks]], axis=1)
    below = lax.broadcasted_iota(jnp.int32, factors.shape, 0)
    here = lax.broadcasted_iota(jnp.int32, solving.shape, 0)
    for j in range(total - 1):
        scale = factors[j:j + 1] / factors[j:j + 1, j:j + 1]
        factors = factors - jnp.where(below > j, factors[:, j:j + 1], 0.0) * scale
        if j < size:
            pivot = solving[j:j + 1] / solving[j:j + 1, j:j + 1]
            solving = jnp.where(here == j, pivot, solving - solving[:, j:j + 1] * pivot)
    pivots = jnp.sum(factors[:, :total] * eye, axis=1, keepdims=True)
    factors = factors / jnp.sqrt(pivots)
    upper = jnp.where(row <= col, factors[:, :total], 0.0)
    inverse = factors[:size, total:total + size]
    hessenberg = contract(inverse, contract(shift, upper, 1, 1), 1, 0)
    row = lax.broadcasted_iota(jnp.int32, hessenberg.shape, 0) // blocks
    col = lax.broadcasted_iota(jnp.int32, hessenberg.shape, 1) // blocks
    return jnp.where(col <= row + 1, hessenberg, 0.0), solving[:, size:], fit


def blend(buffer, terms, splat, blocks, half, width):
    def tile(step, carry):
        at = pl.multiple_of(step * 8, 8)
        parts = [pl.ds(128 * c, 128) for c in range(width // 128)]
        sums = [[None] * len(parts) for _ in range(blocks)]
        for k, term in enumerate(terms):
            for v in range(blocks):
                values = [term[v, pl.ds(at, 8), lanes] for lanes in parts]
                for w in range(blocks):
                    scale = jnp.broadcast_to(splat[w, pl.ds(k * blocks + v, 1), :], (8, 128))
                    for c, value in enumerate(values):
                        value = scale * value
                        sums[w][c] = value if sums[w][c] is None else sums[w][c] + value
        for w in range(blocks):
            for c, lanes in enumerate(parts):
                buffer[w, pl.ds(at, 8), lanes] = sums[w][c]
        return carry

    lax.fori_loop(0, half // 8, tile, 0)


def place_of(n, half):
    parity = lax.rem(lax.axis_index("gz"), 2)
    layer = (parity, 1 - parity, 1 - parity, parity)[n]
    rows = (parity, parity, 1 - parity, 1 - parity)[n]
    return layer, pl.ds(pl.multiple_of(rows * half, 8), half)


TERMS = (((0, None), (1, None), (2, 0)), ((3, None), (4, None), (2, 1)),
         ((5, None), (6, 0), (7, 0), (8, None)))


def finish_kernel(parts, rows, cols, shift, *refs, blocks, half, width):
    arrays, (hess_out, splat, out, again_out, affine_out, source, buffer, sems, out_sems) = refs[:9], refs[9:]
    copies = []
    middle = blocks // 2
    for n, terms in enumerate(TERMS):
        for k, (ref, at) in enumerate(terms):
            ref = arrays[ref] if at is None else arrays[ref].at[at]
            place = source.at[n, k]
            if ref.shape[0] == middle:
                place = source.at[n, 1, pl.ds(0 if k == 1 else middle, middle)]
            elif k == ITERS:
                place = source.at[n, ITERS - 1]
            count = min(blocks, ref.shape[0])
            copy = pltpu.make_async_copy(ref.at[pl.ds(0, count), pl.ds(0, half)], place, sems.at[n, k])
            copy.start()
            copies.append(copy)
    hessenberg, weights, (again, mean, spread) = solve_small(parts[...], rows, cols, shift[...], blocks)
    again_out[0, 0] = again
    affine_out[0, 0] = mean
    affine_out[0, 1] = spread
    hess_out[...] = hessenberg
    for w in range(blocks):
        splat[w] = jnp.broadcast_to(weights[:, w:w + 1], (ITERS * blocks, 128))
    for copy in copies:
        copy.wait()
    sends = []
    for n in range(len(TERMS)):
        blend(buffer.at[n], [source.at[n, k] for k in range(ITERS)], splat, blocks, half, width)
        layer, at = place_of(n, half)
        sends.append(pltpu.make_async_copy(buffer.at[n], out.at[:, layer, at], out_sems.at[n]))
        sends[-1].start()
    for send in sends:
        send.wait()


def others_kernel(splat, zero, one_first, one_second, two, _, out, source, buffer, sems, out_sem, *,
                  blocks, half, width):
    middle = blocks // 2
    loads = []
    for n, (term, at) in enumerate((
        (zero.at[pl.ds(0, blocks), pl.ds(0, half)], source.at[0]),
        (one_first.at[1], source.at[1, pl.ds(0, middle)]),
        (one_second.at[1], source.at[1, pl.ds(middle, middle)]),
        (two, source.at[2]),
    )):
        loads.append(pltpu.make_async_copy(term, at, sems.at[n]))
        loads[-1].start()
    for load in loads:
        load.wait()
    blend(buffer, [source.at[k] for k in range(ITERS)], splat, blocks, half, width)
    layer, at = place_of(len(TERMS), half)
    send = pltpu.make_async_copy(buffer, out.at[:, layer, at], out_sem)
    send.start()
    send.wait()


def in_hbm(array):
    return pltpu.with_memory_space_constraint(array, pltpu.HBM)


def finish(parts, arrays, blocks, half, width, affine):
    vmem = pl.BlockSpec(memory_space=pltpu.VMEM)
    hbm = pl.BlockSpec(memory_space=pltpu.HBM)
    smem = pl.BlockSpec(memory_space=pltpu.SMEM)
    rows, cols = moment_tables(blocks)
    tables = shift_tables(blocks)
    if affine is None:
        shift = (SPREAD * tables[0] + CENTER * tables[1]).astype(np.float32)
    else:
        shift = tables[0] / affine[0, 1] + tables[1] * affine[0, 0]
    size = ITERS * blocks
    piece = (blocks, half, width)
    return pl.pallas_call(
        functools.partial(finish_kernel, blocks=blocks, half=half, width=width),
        out_shape=(
            jax.ShapeDtypeStruct((size, size + blocks), jnp.float32),
            jax.ShapeDtypeStruct((blocks, size, 128), jnp.float32),
            jax.ShapeDtypeStruct((blocks, 2, 2 * half, width), jnp.float32),
            jax.ShapeDtypeStruct((1, 1), jnp.int32),
            jax.ShapeDtypeStruct((1, 2), jnp.float32),
        ),
        in_specs=[vmem] * 4 + [hbm] * 6 + [pl.BlockSpec(memory_space=pl.ANY)] * 3,
        out_specs=(vmem, vmem, hbm, smem, smem),
        scratch_shapes=[
            pltpu.VMEM((len(TERMS), ITERS, *piece), jnp.float32),
            pltpu.VMEM((len(TERMS), *piece), jnp.float32),
            pltpu.SemaphoreType.DMA((len(TERMS), ITERS + 1)),
            pltpu.SemaphoreType.DMA((len(TERMS),)),
        ],
        compiler_params=pltpu.CompilerParams(vmem_limit_bytes=16 << 20),
        cost_estimate=pl.CostEstimate(flops=300 * blocks * half * width, bytes_accessed=1 << 23, transcendentals=0),
        name="finish",
    )(parts, rows, cols.astype(jnp.bfloat16), shift, *[in_hbm(array) for array in arrays[:6]], *arrays[6:])


def others(splat, zero, one_first, one_second, two, result, half, width):
    vmem = pl.BlockSpec(memory_space=pltpu.VMEM)
    hbm = pl.BlockSpec(memory_space=pltpu.HBM)
    blocks = two.shape[0]
    return pl.pallas_call(
        functools.partial(others_kernel, blocks=blocks, half=half, width=width),
        out_shape=jax.ShapeDtypeStruct(result.shape, result.dtype),
        in_specs=[vmem, hbm] + [pl.BlockSpec(memory_space=pl.ANY)] * 3 + [hbm],
        out_specs=hbm,
        scratch_shapes=[
            pltpu.VMEM((ITERS, blocks, half, width), jnp.float32),
            pltpu.VMEM((blocks, half, width), jnp.float32),
            pltpu.SemaphoreType.DMA((4,)),
            pltpu.SemaphoreType.DMA,
        ],
        input_output_aliases={5: 0},
        compiler_params=pltpu.CompilerParams(vmem_limit_bytes=8 << 20),
        name="others",
    )(splat, in_hbm(zero), one_first, one_second, two, result)


def attempt(right_side, diagonal, affine=None):
    blocks, _, ny, width = right_side.shape
    half = ny // 2
    peers_z, peers_y = lax.axis_size("gz"), lax.axis_size("gy")
    even = lax.axis_index("gz") % 2 == 0
    field = jnp.concatenate([right_side, diagonal[None]], axis=0)
    above = lax.ppermute(field[:, :, ny - EDGE:], "gy", pairs(peers_y, 1))
    under = lax.ppermute(field[:, :, :EDGE], "gy", pairs(peers_y, -1))
    first = jnp.concatenate([field[:, :, :half + EDGE], above], axis=2)
    second = jnp.concatenate([field[:, :, half:], under, field[:, :, half - EDGE:half]], axis=2)

    swap = swap_pairs(peers_z, 1)
    inward = [(i, j) for i, j in pairs(peers_z, 2) if i % 2 == 0] + [(i, j) for i, j in pairs(peers_z, -2) if i % 2]
    outward = [(j, i) for i, j in inward]
    send_near = jnp.where(even, second[:, 1], first[:, 0])
    send_far = jnp.where(even, second[:, 0], first[:, 1])
    keep_near = jnp.where(even, first[:, 1], second[:, 0])
    keep_far = jnp.where(even, first[:, 0], second[:, 1])
    zero, first_step, early, late = kernels(blocks, half, width, peers_z * peers_y, affine)

    def move(array, links):
        return lax.ppermute(array, "gz", links)

    middle = blocks // 2
    got_near = move(send_near, swap)
    in_one = move(keep_near[:blocks, :half], inward)
    out_one = move(keep_far, outward)
    far_a = move(jnp.concatenate([send_far[:middle], send_far[blocks:]], axis=0), swap)
    far_b = move(send_far[middle:blocks], swap)
    out_two = move(keep_near, outward)
    in_two = move(got_near, inward)
    out_a = move(got_near[:middle, :half], outward)
    out_b = move(got_near[middle:blocks, :half], outward)
    nu_zero = zero((keep_far, keep_near), (4, 5), False)
    mid_a, sent_a = first_step((keep_near, got_near, far_a, far_a, out_one), 0)
    back_a = move(sent_a, swap)
    in_a = move(far_a, inward)
    nu_zero = zero((got_near, nu_zero), (6,), True)
    mid_b, sent_b = first_step((keep_near, got_near, far_a, far_b, out_one), 1)
    back_b = move(sent_b, swap)
    in_b = move(far_b, inward)
    near1, near2, near_sent, far_sent, start, x1_near = early(
        keep_far, keep_near, got_near, far_a, far_b, out_one, out_two, mid_a, mid_b, nu_zero)
    near_back2 = move(near_sent, swap)
    first_half = late((in_one, in_two, in_a, keep_far, keep_near, got_near, far_a, far_b, out_one, out_two,
                       out_a, mid_a, mid_b, near1, near2), 0)
    x1_far, x2, nu = late((in_one, in_two, in_b, keep_far, keep_near, got_near, far_a, far_b, out_one, out_two,
                           out_b, mid_a, mid_b, near1, near2, in_a, *first_half, start), 1)
    parts = lax.all_to_all(nu, ("gz", "gy"), 0, 0)
    far_back2 = move(far_sent, swap)
    hessenberg, splat, result, again, fit = finish(
        parts, (keep_far, x1_far, x2, keep_near, x1_near, send_near, back_a, back_b, near_back2), blocks, half, width, affine)
    result = others(splat, send_far, back_a, back_b, far_back2, result, half, width)
    return result, hessenberg, again, fit


def body(right_side, diagonal):
    result, hessenberg, again, fit = attempt(right_side, diagonal)

    def repeat(right_side, diagonal, fit, result, hessenberg):
        affine = jnp.stack([CENTER + SPREAD * fit[0, 0], 1.0 / (SPREAD * fit[0, 1])]).reshape(1, 2)
        return attempt(right_side, diagonal, affine)[:2]

    def accept(right_side, diagonal, fit, result, hessenberg):
        return result, hessenberg

    return lax.cond(again[0, 0] != 0, repeat, accept, right_side, diagonal, fit, result, hessenberg)


def solution(mesh):
    in_specs = (P(None, "gz", "gy", None), P("gz", "gy", None))
    out_specs = (P(None, "gz", "gy", None), P())

    return jax.shard_map(body, mesh=mesh, in_specs=in_specs, out_specs=out_specs, check_vma=False)
```
